256 devices in a mesh: rp: 8 (over x, z_lo), pb: 32 (over z_hi, y, core).
Axes of the slice: x: 4, y: 4, z: 8 (z_hi: 4, z_lo: 2; z = z_hi * 2 + z_lo), core: 2. Of those that a mesh axis runs over, the one named last changes fastest.
Arguments:
- wannier_g: bfloat16 [2, 1024, 32, 1152], P(None, 'rp', 'pb'), may hold values from -0.19921875 to 0.19921875
- rp_coords: int32 [3, 1024], replicated, may hold values from -8 to 8
- q_coords: int32 [3, 512], P(None, ('rp', 'pb')), may hold values from 0 to 15
- k_index: int32 [1], replicated, may hold values from 0 to 7
- k_vectors: bfloat16 [8, 2, 32, 32], replicated, may hold values from -0.75 to 0.75
- kq_vectors: bfloat16 [512, 2, 32, 32], P(('rp', 'pb')), may hold values from -0.75 to 0.75
- modes: bfloat16 [512, 2, 36, 36], P(('rp', 'pb')), may hold values from -0.75 to 0.75
Outputs:
- rotated: float32 [512, 2, 32, 1152], P(('rp', 'pb'))
The draws below stay inside these ranges and needn't reach their ends.
All inputs are finite; a program needn't handle non-finite values.
Results may differ from the reference program's by a relative error of at most 0.0054.
Values may be sent and summed in bfloat16 or wider, within the bound.
No kernel may reach another device: no remote copies, remote signals or barrier semaphores. Data moves between devices by JAX's collectives and lax.ppermute only.
A program may use at most 64 MiB of HBM per device.

```python
import math
import jax
import jax.numpy as jnp
from jax import lax

NB = 32
NM = 36
NR = 1024
NK = 16
KB = 8
Q_DEV = 2
Q = 512
N_RP = 8
N_PB = 32


def with_ends(entries, stream_key, least, largest):
    longest = entries.shape.index(max(entries.shape))
    spots = []
    for shift in (0, 1):
        where = [jax.random.randint(jax.random.fold_in(stream_key, axis), (), 0, length) for axis, length in enumerate(entries.shape)]
        where[longest] = (where[longest] + shift) % entries.shape[longest]
        spots.append(tuple(where))
    return entries.at[spots[0]].set(least).at[spots[1]].set(largest)


def levels(own_key, dims, cuts, low, largest):
    def one(axis_at, parts):
        heights = jax.random.uniform(jax.random.fold_in(jax.random.fold_in(own_key, 6), axis_at), (parts,), jnp.float32, low / len(cuts), largest / len(cuts))
        return jnp.repeat(jnp.exp(heights), dims[axis_at] // parts).reshape((-1,) + (1,) * (len(dims) - axis_at - 1))

    factor_of = one(*cuts[0])
    for cut in cuts[1:]:
        factor_of = factor_of * one(*cut)
    return factor_of


def centred(key, extent, width, most, split=(), dtype=jnp.bfloat16):
    values = width * jax.random.normal(key, extent, jnp.float32)
    if split:
        values = values * levels(key, extent, split, -0.22, 0.18)
    return jnp.clip(values, -most, most).astype(dtype)


def setup_inputs(seed: int = 0) -> dict:
    streams_of = jax.random.split(jax.random.key(seed), 8)
    return {
        "wannier_g": centred(streams_of[0], (2, NR, NB, NB * NM), 0.03, 0.19921875, ((1, 8), (2, 32))),
        "rp_coords": with_ends(jax.random.randint(streams_of[1], (3, NR), -8, 9), jax.random.fold_in(streams_of[1], 1), -8, 8).astype(jnp.int32),
        "q_coords": with_ends(jax.random.randint(streams_of[2], (3, Q), 0, NK), jax.random.fold_in(streams_of[2], 1), 0, NK - 1).astype(jnp.int32),
        "k_index": jax.random.randint(streams_of[3], (1,), 0, KB).astype(jnp.int32),
        "k_vectors": centred(streams_of[4], (KB, 2, NB, NB), (2 * NB) ** -0.5, 0.75),
        "kq_vectors": centred(streams_of[5], (Q, 2, NB, NB), (2 * NB) ** -0.5, 0.75, ((0, 256),)),
        "modes": centred(streams_of[6], (Q, 2, NM, NM), (2 * NM) ** -0.5, 0.75, ((0, 256),)),
    }


def phases(q_rows, r_coords):
    turns = jnp.mod(jnp.sum(q_rows[:, :, None] * r_coords[:, None, :], axis=0), NK)
    angle = turns.astype(jnp.float32) * (2.0 * math.pi / NK)
    cosine = jnp.cos(angle).astype(jnp.bfloat16)
    sine = jnp.sin(angle).astype(jnp.bfloat16)
    return jnp.concatenate([cosine, -sine], axis=1), jnp.concatenate([sine, cosine], axis=1)


def rotate(fourier, mode_vecs, unit, kq_vecs):
    count = fourier.shape[0]
    field = fourier.reshape(count, 2, NB, NB, NM).astype(jnp.float32)
    e_real, e_imag = mode_vecs[:, 0], mode_vecs[:, 1]
    e_block = jnp.stack([jnp.stack([e_real, e_imag], 2), jnp.stack([-e_imag, e_real], 2)], 1).astype(jnp.float32)
    by_mode = jnp.einsum("qcmnv,qcvdu->qdmnu", field, e_block).astype(jnp.bfloat16)
    u_real, u_imag = unit[0], unit[1]
    u_block = jnp.stack([jnp.stack([u_real, u_imag], 1), jnp.stack([-u_imag, u_real], 1)], 0).astype(jnp.float32)
    by_band = jnp.einsum("qcmnu,cndj->qdmju", by_mode.astype(jnp.float32), u_block).astype(jnp.bfloat16)
    v_real, v_imag = kq_vecs[:, 0], kq_vecs[:, 1]
    v_block = jnp.stack([jnp.stack([v_real, -v_imag], 2), jnp.stack([v_imag, v_real], 2)], 1).astype(jnp.float32)
    result = jnp.einsum("qcmju,qcmdi->qdiju", by_band.astype(jnp.float32), v_block)
    return result.reshape(count, 2, NB, NB * NM)


def reference(wannier_g, rp_coords, q_coords, k_index, k_vectors, kq_vectors, modes):
    blocks = N_RP * N_PB
    right = wannier_g.reshape(2 * NR, NB * NB * NM)
    unit = lax.dynamic_index_in_dim(k_vectors, k_index[0], 0, keepdims=False)
    q_blocks = q_coords.reshape(3, blocks, Q_DEV).transpose(1, 0, 2)
    mode_blocks = modes.reshape(blocks, Q_DEV, 2, NM, NM)
    kq_blocks = kq_vectors.reshape(blocks, Q_DEV, 2, NB, NB)

    def one_block(items):
        q_rows, mode_vecs, kq_vecs = items
        left_real, left_imag = phases(q_rows, rp_coords)
        f_real = jnp.dot(left_real, right, preferred_element_type=jnp.float32).astype(jnp.bfloat16)
        f_imag = jnp.dot(left_imag, right, preferred_element_type=jnp.float32).astype(jnp.bfloat16)
        fourier = jnp.stack([f_real, f_imag], 1)
        return rotate(fourier, mode_vecs, unit, kq_vecs)

    result = lax.map(one_block, (q_blocks, mode_blocks, kq_blocks))
    return result.reshape(Q, 2, NB, NB * NM)
```

```python
import math

import jax
import jax.numpy as jnp
from jax import lax
from jax.sharding import PartitionSpec as P

NK = 16


def in_blocks(x, dim, length):
    shape = x.shape
    parts = x.reshape(*shape[:dim], length, shape[dim] // length, *shape[dim + 1 :])
    return jnp.moveaxis(parts, dim, 0)


def joined_along(parts, dim):
    shape = list(parts.shape[1:])
    shape[dim] *= parts.shape[0]
    return jnp.moveaxis(parts, 0, dim).reshape(shape)


def one_exchange(x, axis, axes, splits, concats):
    sizes = [lax.axis_size(a) for a in axes]
    parts = in_blocks(x, splits[0], sizes[0])
    parts = jnp.moveaxis(in_blocks(parts, splits[1] + 1, sizes[1]), 0, 1)
    inside = parts.shape[2:]
    parts = parts.reshape(-1, *inside)
    parts = lax.all_to_all(parts, axis, split_axis=0, concat_axis=0, tiled=True)
    parts = joined_along(parts.reshape(*sizes, *inside), concats[0] + 1)
    return joined_along(parts, concats[1])


def phases(q_rows, r_coords):
    turns = jnp.mod(jnp.sum(q_rows[:, :, None] * r_coords[:, None, :], axis=0), NK)
    angle = turns.astype(jnp.float32) * (2.0 * math.pi / NK)
    cosine = jnp.cos(angle).astype(jnp.bfloat16)
    sine = jnp.sin(angle).astype(jnp.bfloat16)
    return (jnp.concatenate([cosine, -sine], axis=1), jnp.concatenate([sine, cosine], axis=1))


def rotate(fourier, mode_vecs, unit, kq_vecs):
    count = fourier.shape[0]
    bands = kq_vecs.shape[2]
    branches = mode_vecs.shape[2]
    field = fourier.reshape(count, 2, bands, bands, branches)
    e_real, e_imag = (mode_vecs[:, 0], mode_vecs[:, 1])
    e_block = jnp.stack([jnp.stack([e_real, e_imag], 2), jnp.stack([-e_imag, e_real], 2)], 1)
    by_mode = jnp.einsum(
        "qcmnv,qcvdu->qdmnu", field, e_block, preferred_element_type=jnp.float32
    ).astype(jnp.bfloat16)
    u_real, u_imag = (unit[0], unit[1])
    u_block = jnp.stack([jnp.stack([u_real, u_imag], 1), jnp.stack([-u_imag, u_real], 1)], 0)
    by_band = jnp.einsum(
        "qcmnu,cndj->qdmju", by_mode, u_block, preferred_element_type=jnp.float32
    ).astype(jnp.bfloat16)
    v_real, v_imag = (kq_vecs[:, 0], kq_vecs[:, 1])
    v_block = jnp.stack([jnp.stack([v_real, -v_imag], 2), jnp.stack([v_imag, v_real], 2)], 1)
    result = jnp.einsum("qcmju,qcmdi->qdiju", by_band, v_block, preferred_element_type=jnp.float32)
    return result.reshape(count, 2, bands, bands * branches)


def local(wannier_g, rp_coords, q_coords, k_index, k_vectors, kq_vectors, modes):
    devices = lax.axis_size("rp") * lax.axis_size("pb")
    per_device = q_coords.shape[1]
    sent = jnp.broadcast_to(q_coords.T[None], (devices, per_device, 3))
    q_all = lax.all_to_all(sent, ("rp", "pb"), split_axis=0, concat_axis=0, tiled=True)
    total = devices * per_device
    q_rows = q_all.reshape(total, 3).T
    moved = lax.all_to_all(wannier_g, "rp", split_axis=3, concat_axis=1, tiled=True)
    right = moved.reshape(2 * moved.shape[1], -1)
    left_real, left_imag = phases(q_rows, rp_coords)
    f_real = jnp.dot(left_real, right, preferred_element_type=jnp.float32).astype(jnp.bfloat16)
    f_imag = jnp.dot(left_imag, right, preferred_element_type=jnp.float32).astype(jnp.bfloat16)
    fourier = jnp.stack([f_real, f_imag], 1).reshape(total, 2, moved.shape[2], moved.shape[3])
    owned = one_exchange(fourier, ("rp", "pb"), ("rp", "pb"), (0, 0), (3, 2))
    select = (jnp.arange(k_vectors.shape[0]) == k_index[0]).astype(jnp.bfloat16)
    unit = jnp.einsum("k,kcnj->cnj", select, k_vectors, preferred_element_type=jnp.float32).astype(
        jnp.bfloat16
    )
    return rotate(owned, modes, unit, kq_vectors)


def solution(mesh):
    return jax.shard_map(
        local,
        mesh=mesh,
        in_specs=(
            P(None, "rp", "pb", None),
            P(),
            P(None, ("rp", "pb")),
            P(),
            P(),
            P(("rp", "pb"), None, None, None),
            P(("rp", "pb"), None, None, None),
        ),
        out_specs=P(("rp", "pb"), None, None, None),
        check_vma=False,
    )
```

```python
import math

import jax
import jax.numpy as jnp
import numpy as np
from jax import lax
from jax.experimental import pallas as pl
from jax.experimental.pallas import tpu as pltpu
from jax.sharding import PartitionSpec as P

NK = 16
LANES = 128
EXTRA = 16
BANDS = 32
BRANCHES = 36
SLOT = 64
AXES = ("rp", "pb")


def sine_series():
    points = np.arange(1, 5) / NK
    powers = np.stack([points ** (2 * k) for k in range(4)], 1)
    values = np.sin(2 * math.pi * points) / points
    return [float(c) for c in np.linalg.solve(powers, values)]


SERIES = sine_series()


def lane_of(shape):
    return lax.broadcasted_iota(jnp.int32, shape, len(shape) - 1)


def turned(x, shift):
    shift %= LANES
    return pltpu.roll(x, shift, 1) if shift else x


def pack_kernel(w_ref, o_ref):
    groups = o_ref.shape[0]
    rows = w_ref.shape[0]
    cut = rows * EXTRA // LANES
    pieces = rows // cut
    for a in range(groups):
        o_ref[a, :rows, :] = w_ref[:, a * LANES : (a + 1) * LANES]
        o_ref[a, rows + cut :, :] = jnp.zeros((o_ref.shape[1] - rows - cut, LANES), o_ref.dtype)
    tail = w_ref[:, groups * LANES :].astype(jnp.float32)
    lane = lane_of((cut, LANES))
    half = pieces // 2
    for a in range(groups):
        mixed = jnp.zeros((cut, LANES), jnp.float32)
        for j in range(pieces):
            place = 2 * (j % half) + j // half
            piece = turned(tail[j * cut : (j + 1) * cut], EXTRA * (place - a))
            mixed = jnp.where(lane // EXTRA == place, piece, mixed)
        o_ref[a, rows : rows + cut, :] = mixed.astype(o_ref.dtype)


def wave(u):
    w = 0.25 - jnp.abs(u - jnp.round(u))
    s = w * w
    value = SERIES[3]
    for c in SERIES[2::-1]:
        value = value * s + c
    return value * w


def fourier_kernel(x_ref, r_ref, o_ref, left, right):
    groups = x_ref.shape[0]
    span = r_ref.shape[1] // groups
    vectors = groups * span
    rows = 2 * span
    cut = rows * EXTRA // LANES
    half = span // cut
    lane = lane_of((cut, LANES))
    per_group = left.shape[0] // groups
    r_all = r_ref[...]
    for a in range(groups):
        coords = x_ref[a, rows + cut :, :].astype(jnp.float32)
        q_rows = coords.T[:per_group].astype(jnp.bfloat16)
        turns = jnp.dot(q_rows, r_all, preferred_element_type=jnp.float32)
        at = slice(a * per_group, (a + 1) * per_group)
        left[at, :vectors] = wave(turns).astype(jnp.bfloat16)
        left[at, vectors:] = wave(turns - 0.25).astype(jnp.bfloat16)
    for a in range(groups):
        real = x_ref[a, :span, :]
        imag = x_ref[a, span:rows, :]
        top = a * span
        low = vectors + a * span
        right[top : top + span, :LANES] = real
        right[top : top + span, LANES : 2 * LANES] = imag
        right[low : low + span, :LANES] = -imag
        right[low : low + span, LANES : 2 * LANES] = real
        mixed = x_ref[a, rows : rows + cut, :].astype(jnp.float32)
        for j in range(half):
            first = turned(mixed, -2 * EXTRA * j)
            second = jnp.where(lane < EXTRA, -turned(first, -EXTRA), turned(first, EXTRA))
            right[top + j * cut : top + (j + 1) * cut, 2 * LANES :] = first.astype(jnp.bfloat16)
            right[low + j * cut : low + (j + 1) * cut, 2 * LANES :] = second.astype(jnp.bfloat16)
    total = jnp.dot(left[...], right[...], preferred_element_type=jnp.float32)
    for k in range(3):
        part = total[:, k * LANES : (k + 1) * LANES].astype(jnp.bfloat16)
        o_ref[:, k] = part.reshape(o_ref.shape[0], 2, LANES)


def rotate_kernel(x_ref, v_ref, e_ref, u_ref, o_ref, spread, mixed):
    groups = x_ref.shape[0]
    pairs = 2 * BANDS
    lane = lane_of((pairs, LANES))
    tiles = []
    for a in range(groups):
        tiles.append(jnp.concatenate([x_ref[a, 0], x_ref[a, 1]], 0))
    tails = [x_ref[a, 2].astype(jnp.float32) for a in range(groups)]
    parts = []
    for c in range(2):
        part = jnp.zeros((pairs, LANES), jnp.float32)
        for a in range(groups):
            part = jnp.where(lane // EXTRA == a, turned(tails[a], EXTRA * (a - c)), part)
        parts.append(part.astype(jnp.bfloat16))
    tiles.append(jnp.concatenate(parts, 0))
    field = [jnp.dot(v_ref[...], t, preferred_element_type=jnp.float32) for t in tiles]

    lane = lane_of((BANDS, LANES))
    for q in range(2):
        for n in range(BANDS):
            t, s = divmod(BRANCHES * n, LANES)
            halves = []
            for c in range(2):
                at = slice((2 * q + c) * BANDS, (2 * q + c + 1) * BANDS)
                piece = field[t][at]
                if s + BRANCHES > LANES:
                    piece = jnp.where(lane >= s, piece, field[t + 1][at])
                halves.append(turned(piece, SLOT * c - s))
            spread[q, pl.ds(n, BANDS, stride=BANDS), :] = jnp.where(lane < SLOT, halves[0], halves[1])

    modes_done = [
        jnp.dot(spread[q].astype(jnp.bfloat16), e_ref[q], preferred_element_type=jnp.float32).astype(
            jnp.bfloat16
        )
        for q in range(2)
    ]
    block = u_ref.shape[1]
    for g in range(BANDS * BANDS // block):
        at = slice(g * block, (g + 1) * block)
        plain = jnp.concatenate([modes_done[0][at, :LANES], modes_done[1][at, :LANES]], 1)
        turned_by_i = jnp.concatenate([modes_done[0][at, LANES:], modes_done[1][at, LANES:]], 1)
        done = jnp.dot(u_ref[0], plain, preferred_element_type=jnp.float32) + jnp.dot(
            u_ref[1], turned_by_i, preferred_element_type=jnp.float32
        )
        for q in range(2):
            mixed[q, at, :] = done[:, q * LANES : (q + 1) * LANES]

    for q in range(2):
        for c in range(2):
            out = None
            for j in range(BANDS):
                t, s = divmod(BRANCHES * j, LANES)
                piece = mixed[q, pl.ds(j, BANDS, stride=BANDS), :]
                piece = turned(piece, s - SLOT * c)
                out = piece if out is None else jnp.where(lane >= s, piece, out)
                if s + BRANCHES >= LANES:
                    o_ref[q, c, :, t * LANES : (t + 1) * LANES] = out
                    out = piece if s + BRANCHES > LANES else None


def room(mib):
    return pltpu.CompilerParams(vmem_limit_bytes=mib * 2**20)


def vmem(shape, dtype):
    return jax.ShapeDtypeStruct(shape, dtype)


def complex_block(real, imag):
    return jnp.stack([jnp.stack([real, imag], 1), jnp.stack([-imag, real], 1)], 0)


def local(wannier_g, rp_coords, q_coords, k_index, k_vectors, kq_vectors, modes):
    groups = lax.axis_size("rp")
    columns = lax.axis_size("pb")
    devices = groups * columns
    per_device = q_coords.shape[1]
    span = wannier_g.shape[1]
    rows = 2 * span
    cut = rows * EXTRA // LANES
    chunk = rows + cut + 8

    with jax.named_scope("coords"):
        sent = jnp.broadcast_to(q_coords.astype(jnp.bfloat16)[None], (columns, 3, per_device))
        near = lax.all_to_all(sent, "pb", split_axis=0, concat_axis=0, tiled=True)
        near = near.transpose(1, 0, 2).reshape(3, columns * per_device)
        near = jnp.pad(near, ((0, 5), (0, LANES - columns * per_device)))
    with jax.named_scope("pack"):
        packed = pl.pallas_call(
            pack_kernel,
            out_shape=vmem((groups, chunk, LANES), jnp.bfloat16),
            compiler_params=room(8),
            name="pack",
        )(wannier_g.reshape(rows, wannier_g.shape[3]))
        packed = packed.at[:, rows + cut :, :].set(jnp.broadcast_to(near, (groups, 8, LANES)))
    with jax.named_scope("wannier"):
        moved = lax.all_to_all(packed, "rp", split_axis=0, concat_axis=0, tiled=True)

    turns_of = jnp.pad(rp_coords.astype(jnp.float32) / NK, ((0, 5), (0, 0))).astype(jnp.bfloat16)
    vectors = rp_coords.shape[1]
    total = devices * per_device
    with jax.named_scope("fourier"):
        fourier = pl.pallas_call(
            fourier_kernel,
            out_shape=vmem((devices, 3, per_device, LANES), jnp.bfloat16),
            scratch_shapes=[
                pltpu.VMEM((total, 2 * vectors), jnp.bfloat16),
                pltpu.VMEM((2 * vectors, 3 * LANES), jnp.bfloat16),
            ],
            compiler_params=room(16),
            name="fourier",
        )(moved, turns_of)
    with jax.named_scope("owners"):
        owned = lax.all_to_all(fourier, AXES, split_axis=0, concat_axis=0, tiled=True)
        owned = owned.reshape(groups, columns, 3, per_device, LANES).transpose(0, 2, 1, 3, 4)
        owned = owned.reshape(groups, 3, columns * per_device, LANES)

    with jax.named_scope("tables"):
        select = (jnp.arange(k_vectors.shape[0]) == k_index[0]).astype(jnp.bfloat16)
        unit = jnp.einsum("k,kcnj->cnj", select, k_vectors, preferred_element_type=jnp.float32)
        eight = jnp.eye(8, dtype=jnp.float32)
        u_table = jnp.einsum("ab,cnj->cajbn", eight, unit).reshape(2, 8 * BANDS, 8 * BANDS)
        u_table = u_table.astype(jnp.bfloat16)
        v_real, v_imag = kq_vectors[:, 0], kq_vectors[:, 1]
        v_block = jnp.stack([jnp.stack([v_real, -v_imag], 2), jnp.stack([v_imag, v_real], 2)], 1)
        own = jnp.eye(per_device, dtype=jnp.bfloat16)
        v_table = v_block.transpose(0, 3, 4, 1, 2)[..., None] * own[:, None, None, None, None, :]
        v_table = v_table.reshape(per_device * 2 * BANDS, 2 * BANDS * per_device)
        rest = SLOT - BRANCHES
        e_pad = jnp.pad(modes, ((0, 0), (0, 0), (0, rest), (0, rest)))
        e_real, e_imag = e_pad[:, 0], e_pad[:, 1]
        e_table = jnp.concatenate(
            [
                jnp.concatenate([e_real, e_imag, -e_imag, e_real], 2),
                jnp.concatenate([-e_imag, e_real, -e_real, -e_imag], 2),
            ],
            1,
        )
    with jax.named_scope("rotate"):
        return pl.pallas_call(
            rotate_kernel,
            out_shape=vmem((per_device, 2, BANDS, BANDS * BRANCHES), jnp.float32),
            scratch_shapes=[
                pltpu.VMEM((per_device, BANDS * BANDS, LANES), jnp.float32),
                pltpu.VMEM((per_device, BANDS * BANDS, LANES), jnp.float32),
            ],
            compiler_params=room(16),
            name="rotate",
        )(owned, v_table, e_table, u_table)


def solution(mesh):
    return jax.shard_map(
        local,
        mesh=mesh,
        in_specs=(
            P(None, "rp", "pb", None),
            P(),
            P(None, AXES),
            P(),
            P(),
            P(AXES, None, None, None),
            P(AXES, None, None, None),
        ),
        out_specs=P(AXES, None, None, None),
        check_vma=False,
    )
```

```python
import math

import jax
import jax.numpy as jnp
import numpy as np
from jax import lax
from jax.experimental import pallas as pl
from jax.experimental.pallas import tpu as pltpu
from jax.sharding import PartitionSpec as P

NK = 16
LANES = 128
EXTRA = 16
BANDS = 32
BRANCHES = 36
SLOT = 64
AXES = ("rp", "pb")


def sine_series():
    points = np.arange(1, 5) / NK
    powers = np.stack([points ** (2 * k) for k in range(4)], 1)
    values = np.sin(2 * math.pi * points) / points
    return [float(c) for c in np.linalg.solve(powers, values)]


SERIES = sine_series()


def lane_of(shape):
    return lax.broadcasted_iota(jnp.int32, shape, len(shape) - 1)


def turned(x, shift):
    shift %= LANES
    return pltpu.roll(x, shift, 1) if shift else x


def pack_kernel(w_ref, o_ref):
    groups = o_ref.shape[0]
    rows = w_ref.shape[0]
    cut = rows * EXTRA // LANES
    pieces = rows // cut
    for a in range(groups):
        o_ref[a, :rows, :] = w_ref[:, a * LANES : (a + 1) * LANES]
        o_ref[a, rows + cut :, :] = jnp.zeros((o_ref.shape[1] - rows - cut, LANES), o_ref.dtype)
    tail = w_ref[:, groups * LANES :].astype(jnp.float32)
    lane = lane_of((cut, LANES))
    half = pieces // 2
    for a in range(groups):
        mixed = jnp.zeros((cut, LANES), jnp.float32)
        for j in range(pieces):
            place = 2 * (j % half) + j // half
            piece = turned(tail[j * cut : (j + 1) * cut], EXTRA * (place - a))
            mixed = jnp.where(lane // EXTRA == place, piece, mixed)
        o_ref[a, rows : rows + cut, :] = mixed.astype(o_ref.dtype)


def wave(u):
    w = 0.25 - jnp.abs(u - jnp.round(u))
    s = w * w
    value = SERIES[3]
    for c in SERIES[2::-1]:
        value = value * s + c
    return value * w


def fourier_kernel(x_ref, r_ref, o_ref, left, right):
    groups = x_ref.shape[0]
    span = r_ref.shape[1] // groups
    vectors = groups * span
    rows = 2 * span
    cut = rows * EXTRA // LANES
    half = span // cut
    lane = lane_of((cut, LANES))
    per_group = left.shape[0] // groups
    r_all = r_ref[...]
    for a in range(groups):
        coords = x_ref[a, rows + cut :, :].astype(jnp.float32)
        q_rows = coords.T[:per_group].astype(jnp.bfloat16)
        turns = jnp.dot(q_rows, r_all, preferred_element_type=jnp.float32)
        at = slice(a * per_group, (a + 1) * per_group)
        left[at, :vectors] = wave(turns).astype(jnp.bfloat16)
        left[at, vectors:] = wave(turns - 0.25).astype(jnp.bfloat16)
    for a in range(groups):
        real = x_ref[a, :span, :]
        imag = x_ref[a, span:rows, :]
        top = a * span
        low = vectors + a * span
        right[top : top + span, :LANES] = real
        right[top : top + span, LANES : 2 * LANES] = imag
        right[low : low + span, :LANES] = -imag
        right[low : low + span, LANES : 2 * LANES] = real
        mixed = x_ref[a, rows : rows + cut, :].astype(jnp.float32)
        for j in range(half):
            first = turned(mixed, -2 * EXTRA * j)
            second = jnp.where(lane < EXTRA, -turned(first, -EXTRA), turned(first, EXTRA))
            right[top + j * cut : top + (j + 1) * cut, 2 * LANES :] = first.astype(jnp.bfloat16)
            right[low + j * cut : low + (j + 1) * cut, 2 * LANES :] = second.astype(jnp.bfloat16)
    total = jnp.dot(left[...], right[...], preferred_element_type=jnp.float32)
    for k in range(3):
        part = total[:, k * LANES : (k + 1) * LANES].astype(jnp.bfloat16)
        o_ref[:, k] = part.reshape(o_ref.shape[0], 2, LANES)


def rotate_kernel(x_ref, v_ref, e_ref, u_ref, o_ref, spread, mixed):
    groups = x_ref.shape[0]
    pairs = 2 * BANDS
    lane = lane_of((pairs, LANES))
    tiles = []
    for a in range(groups):
        tiles.append(jnp.concatenate([x_ref[a, :, k].reshape(pairs, LANES) for k in range(2)], 0))
    tails = [x_ref[a, :, 2].reshape(pairs, LANES).astype(jnp.float32) for a in range(groups)]
    parts = []
    for c in range(2):
        part = jnp.zeros((pairs, LANES), jnp.float32)
        for a in range(groups):
            part = jnp.where(lane // EXTRA == a, turned(tails[a], EXTRA * (a - c)), part)
        parts.append(part.astype(jnp.bfloat16))
    tiles.append(jnp.concatenate(parts, 0))
    field = [jnp.dot(v_ref[...], t, preferred_element_type=jnp.float32) for t in tiles]

    lane = lane_of((BANDS, LANES))
    for q in range(2):
        for n in range(BANDS):
            t, s = divmod(BRANCHES * n, LANES)
            halves = []
            for c in range(2):
                at = slice((2 * q + c) * BANDS, (2 * q + c + 1) * BANDS)
                piece = field[t][at]
                if s + BRANCHES > LANES:
                    piece = jnp.where(lane >= s, piece, field[t + 1][at])
                halves.append(turned(piece, SLOT * c - s))
            spread[q, pl.ds(n, BANDS, stride=BANDS), :] = jnp.where(lane < SLOT, halves[0], halves[1])

    modes_done = [
        jnp.dot(spread[q].astype(jnp.bfloat16), e_ref[q], preferred_element_type=jnp.float32).astype(
            jnp.bfloat16
        )
        for q in range(2)
    ]
    block = u_ref.shape[1]
    for g in range(BANDS * BANDS // block):
        at = slice(g * block, (g + 1) * block)
        plain = jnp.concatenate([modes_done[0][at, :LANES], modes_done[1][at, :LANES]], 1)
        turned_by_i = jnp.concatenate([modes_done[0][at, LANES:], modes_done[1][at, LANES:]], 1)
        done = jnp.dot(u_ref[0], plain, preferred_element_type=jnp.float32) + jnp.dot(
            u_ref[1], turned_by_i, preferred_element_type=jnp.float32
        )
        for q in range(2):
            mixed[q, at, :] = done[:, q * LANES : (q + 1) * LANES]

    for q in range(2):
        for c in range(2):
            out = None
            for j in range(BANDS):
                t, s = divmod(BRANCHES * j, LANES)
                piece = mixed[q, pl.ds(j, BANDS, stride=BANDS), :]
                piece = turned(piece, s - SLOT * c)
                out = piece if out is None else jnp.where(lane >= s, piece, out)
                if s + BRANCHES >= LANES:
                    o_ref[q, c, :, t * LANES : (t + 1) * LANES] = out
                    out = piece if s + BRANCHES > LANES else None


def room(mib):
    return pltpu.CompilerParams(vmem_limit_bytes=mib * 2**20)


def vmem(shape, dtype):
    return jax.ShapeDtypeStruct(shape, dtype)


def complex_block(real, imag):
    return jnp.stack([jnp.stack([real, imag], 1), jnp.stack([-imag, real], 1)], 0)


def local(wannier_g, rp_coords, q_coords, k_index, k_vectors, kq_vectors, modes):
    groups = lax.axis_size("rp")
    columns = lax.axis_size("pb")
    devices = groups * columns
    per_device = q_coords.shape[1]
    span = wannier_g.shape[1]
    rows = 2 * span
    cut = rows * EXTRA // LANES
    chunk = rows + cut + 8

    with jax.named_scope("coords"):
        sent = jnp.broadcast_to(q_coords[None], (columns, 3, per_device))
        near = lax.all_to_all(sent, "pb", split_axis=0, concat_axis=0, tiled=True)
        near = near.transpose(1, 0, 2).reshape(3, columns * per_device)
        near = jnp.pad(near.astype(jnp.bfloat16), ((0, 5), (0, LANES - columns * per_device)))
    with jax.named_scope("pack"):
        packed = pl.pallas_call(
            pack_kernel,
            out_shape=vmem((groups, chunk, LANES), jnp.bfloat16),
            compiler_params=room(8),
            name="pack",
        )(wannier_g.reshape(rows, wannier_g.shape[3]))
    near, rp_coords, k_index, k_vectors, kq_vectors, modes = lax.optimization_barrier(
        (near, rp_coords, k_index, k_vectors, kq_vectors, modes)
    )
    turns_of = jnp.pad(rp_coords.astype(jnp.float32) / NK, ((0, 5), (0, 0))).astype(jnp.bfloat16)
    with jax.named_scope("tables"):
        select = (jnp.arange(k_vectors.shape[0]) == k_index[0]).astype(jnp.bfloat16)
        unit = jnp.einsum("k,kcnj->cnj", select, k_vectors, preferred_element_type=jnp.float32)
        eight = jnp.eye(8, dtype=jnp.float32)
        u_table = jnp.einsum("ab,cnj->cajbn", eight, unit).reshape(2, 8 * BANDS, 8 * BANDS)
        u_table = u_table.astype(jnp.bfloat16)
        v_real, v_imag = kq_vectors[:, 0], kq_vectors[:, 1]
        v_block = jnp.stack([jnp.stack([v_real, -v_imag], 2), jnp.stack([v_imag, v_real], 2)], 1)
        twice = jnp.repeat(jnp.eye(2 * BANDS, dtype=jnp.bfloat16), per_device, 1)
        v_table = jnp.einsum(
            "qcmdi,cmk->qdik",
            v_block,
            twice.reshape(2, BANDS, 2 * BANDS * per_device),
            preferred_element_type=jnp.float32,
        ).reshape(per_device, 2 * BANDS, 2 * BANDS * per_device)
        own = jnp.arange(2 * BANDS * per_device) % per_device == jnp.arange(per_device)[:, None]
        v_table = jnp.where(own[:, None, :], v_table, 0.0).astype(jnp.bfloat16)
        v_table = v_table.reshape(per_device * 2 * BANDS, 2 * BANDS * per_device)
        rest = SLOT - BRANCHES
        e_pad = jnp.pad(modes, ((0, 0), (0, 0), (0, rest), (0, rest)))
        e_real, e_imag = e_pad[:, 0], e_pad[:, 1]
        e_table = jnp.concatenate(
            [
                jnp.concatenate([e_real, e_imag, -e_imag, e_real], 2),
                jnp.concatenate([-e_imag, e_real, -e_real, -e_imag], 2),
            ],
            1,
        )
    packed = packed.at[:, rows + cut :, :].set(jnp.broadcast_to(near, (groups, 8, LANES)))
    with jax.named_scope("wannier"):
        moved = lax.all_to_all(packed, "rp", split_axis=0, concat_axis=0, tiled=True)

    vectors = rp_coords.shape[1]
    total = devices * per_device
    with jax.named_scope("fourier"):
        fourier = pl.pallas_call(
            fourier_kernel,
            out_shape=vmem((devices, 3, per_device, LANES), jnp.bfloat16),
            scratch_shapes=[
                pltpu.VMEM((total, 2 * vectors), jnp.bfloat16),
                pltpu.VMEM((2 * vectors, 3 * LANES), jnp.bfloat16),
            ],
            compiler_params=room(16),
            name="fourier",
        )(moved, turns_of)
    fourier, u_table, v_table, e_table = lax.optimization_barrier(
        (fourier, u_table, v_table, e_table)
    )
    with jax.named_scope("owners"):
        owned = lax.all_to_all(fourier, AXES, split_axis=0, concat_axis=0, tiled=True)
        owned = owned.reshape(groups, columns, 3, per_device, LANES)

    with jax.named_scope("rotate"):
        return pl.pallas_call(
            rotate_kernel,
            out_shape=vmem((per_device, 2, BANDS, BANDS * BRANCHES), jnp.float32),
            scratch_shapes=[
                pltpu.VMEM((per_device, BANDS * BANDS, LANES), jnp.float32),
                pltpu.VMEM((per_device, BANDS * BANDS, LANES), jnp.float32),
            ],
            compiler_params=room(16),
            name="rotate",
        )(owned, v_table, e_table, u_table)


def solution(mesh):
    return jax.shard_map(
        local,
        mesh=mesh,
        in_specs=(
            P(None, "rp", "pb", None),
            P(),
            P(None, AXES),
            P(),
            P(),
            P(AXES, None, None, None),
            P(AXES, None, None, None),
        ),
        out_specs=P(AXES, None, None, None),
        check_vma=False,
    )
```

```python
import math

import jax
import jax.numpy as jnp
import numpy as np
from jax import lax
from jax.experimental import pallas as pl
from jax.experimental.pallas import tpu as pltpu
from jax.sharding import PartitionSpec as P


NK = 16
LANES = 128
EXTRA = 16
BANDS = 32
BRANCHES = 36
SLOT = 64
AXES = ("rp", "pb")


def sine_series():
    points = np.arange(1, 5) / NK
    powers = np.stack([points ** (2 * k) for k in range(4)], 1)
    values = np.sin(2 * math.pi * points) / points
    return [float(c) for c in np.linalg.solve(powers, values)]


SERIES = sine_series()


def lane_of(shape):
    return lax.broadcasted_iota(jnp.int32, shape, len(shape) - 1)


def turned(x, shift):
    shift %= LANES
    return pltpu.roll(x, shift, 1) if shift else x


def pack_kernel(w_ref, o_ref, tail_ref, cut_ref, sems):
    groups, cut, _ = cut_ref.shape
    rows = w_ref.shape[0]
    pieces = rows // cut
    fetch = pltpu.make_async_copy(w_ref.at[:, groups * LANES :], tail_ref, sems.at[groups])
    fetch.start()
    moves = [
        pltpu.make_async_copy(
            w_ref.at[:, a * LANES : (a + 1) * LANES], o_ref.at[a, :rows, :], sems.at[a]
        )
        for a in range(groups)
    ]
    for move in moves:
        move.start()
    fetch.wait()
    tail = tail_ref[...].astype(jnp.float32)
    lane = lane_of((cut, LANES))
    half = pieces // 2
    for a in range(groups):
        mixed = jnp.zeros((cut, LANES), jnp.float32)
        for j in range(pieces):
            place = 2 * (j % half) + j // half
            piece = turned(tail[j * cut : (j + 1) * cut], EXTRA * (place - a))
            mixed = jnp.where(lane // EXTRA == place, piece, mixed)
        cut_ref[a] = mixed.astype(o_ref.dtype)
    last = pltpu.make_async_copy(cut_ref, o_ref.at[:, rows : rows + cut, :], sems.at[groups + 1])
    last.start()
    for move in moves:
        move.wait()
    last.wait()


def wave(u):
    w = 0.25 - jnp.abs(u - jnp.round(u))
    s = w * w
    value = SERIES[3]
    for c in SERIES[2::-1]:
        value = value * s + c
    return value * w


def fourier_kernel(x_ref, r_ref, o_ref, left, right):
    groups = x_ref.shape[0]
    span = r_ref.shape[1] // groups
    vectors = groups * span
    rows = 2 * span
    cut = rows * EXTRA // LANES
    half = span // cut
    lane = lane_of((cut, LANES))
    per_group = left.shape[0] // groups
    r_all = r_ref[...]
    for a in range(groups):
        coords = x_ref[a, rows + cut :, :].astype(jnp.float32)
        q_rows = coords.T[:per_group].astype(jnp.bfloat16)
        turns = jnp.dot(q_rows, r_all, preferred_element_type=jnp.float32)
        at = slice(a * per_group, (a + 1) * per_group)
        left[at, :vectors] = wave(turns).astype(jnp.bfloat16)
        left[at, vectors:] = wave(turns - 0.25).astype(jnp.bfloat16)
    for a in range(groups):
        real = x_ref[a, :span, :]
        imag = x_ref[a, span:rows, :]
        top = a * span
        low = vectors + a * span
        right[top : top + span, :LANES] = real
        right[top : top + span, LANES : 2 * LANES] = imag
        right[low : low + span, :LANES] = -imag
        right[low : low + span, LANES : 2 * LANES] = real
        mixed = x_ref[a, rows : rows + cut, :].astype(jnp.float32)
        for j in range(half):
            first = turned(mixed, -2 * EXTRA * j)
            second = jnp.where(lane < EXTRA, -turned(first, -EXTRA), turned(first, EXTRA))
            right[top + j * cut : top + (j + 1) * cut, 2 * LANES :] = first.astype(jnp.bfloat16)
            right[low + j * cut : low + (j + 1) * cut, 2 * LANES :] = second.astype(jnp.bfloat16)
    total = jnp.dot(left[...], right[...], preferred_element_type=jnp.float32)
    for k in range(3):
        part = total[:, k * LANES : (k + 1) * LANES].astype(jnp.bfloat16)
        o_ref[:, k] = part.reshape(o_ref.shape[0], 2, LANES)


def rotate_kernel(x_ref, v_ref, e_ref, u_ref, o_ref, spread, mixed, ready, sems):
    groups = x_ref.shape[0]
    pairs = 2 * BANDS
    lane = lane_of((pairs, LANES))
    tiles = []
    for a in range(groups):
        tiles.append(jnp.concatenate([x_ref[a, :, k].reshape(pairs, LANES) for k in range(2)], 0))
    tails = [x_ref[a, :, 2].reshape(pairs, LANES).astype(jnp.float32) for a in range(groups)]
    parts = []
    for c in range(2):
        part = jnp.zeros((pairs, LANES), jnp.float32)
        for a in range(groups):
            part = jnp.where(lane // EXTRA == a, turned(tails[a], EXTRA * (a - c)), part)
        parts.append(part.astype(jnp.bfloat16))
    tiles.append(jnp.concatenate(parts, 0))
    field = [jnp.dot(v_ref[...], t, preferred_element_type=jnp.float32) for t in tiles]

    lane = lane_of((BANDS, LANES))
    modes_done = []
    for q in range(2):
        for n in range(BANDS):
            t, s = divmod(BRANCHES * n, LANES)
            halves = []
            for c in range(2):
                at = slice((2 * q + c) * BANDS, (2 * q + c + 1) * BANDS)
                piece = field[t][at]
                if s + BRANCHES > LANES:
                    piece = jnp.where(lane >= s, piece, field[t + 1][at])
                halves.append(turned(piece, SLOT * c - s))
            both = jnp.where(lane < SLOT, halves[0], halves[1])
            for g in range(BANDS // 8):
                top = 8 * (g * BANDS + n)
                spread[q, top : top + 8, :] = both[8 * g : 8 * (g + 1)]
        done = jnp.dot(
            spread[q].astype(jnp.bfloat16), e_ref[q], preferred_element_type=jnp.float32
        )
        modes_done.append(done.astype(jnp.bfloat16))

    block = u_ref.shape[1]
    for g in range(BANDS * BANDS // block):
        at = slice(g * block, (g + 1) * block)
        plain = jnp.concatenate([modes_done[0][at, :LANES], modes_done[1][at, :LANES]], 1)
        turned_by_i = jnp.concatenate([modes_done[0][at, LANES:], modes_done[1][at, LANES:]], 1)
        done = jnp.dot(u_ref[0], plain, preferred_element_type=jnp.float32) + jnp.dot(
            u_ref[1], turned_by_i, preferred_element_type=jnp.float32
        )
        for q in range(2):
            mixed[q, at, :] = done[:, q * LANES : (q + 1) * LANES]

    sends = []
    for q in range(2):
        for c in range(2):
            out = None
            for j in range(BANDS):
                t, s = divmod(BRANCHES * j, LANES)
                tops = [8 * (g * BANDS + j) for g in range(BANDS // 8)]
                piece = jnp.concatenate([mixed[q, top : top + 8, :] for top in tops], 0)
                piece = turned(piece, s - SLOT * c)
                out = piece if out is None else jnp.where(lane >= s, piece, out)
                if s + BRANCHES >= LANES:
                    ready[q, c, :, t * LANES : (t + 1) * LANES] = out
                    out = piece if s + BRANCHES > LANES else None
            sends.append(pltpu.make_async_copy(ready.at[q, c], o_ref.at[q, c], sems.at[q, c]))
            sends[-1].start()
    for send in sends:
        send.wait()


def room(mib):
    return pltpu.CompilerParams(vmem_limit_bytes=mib * 2**20)


def vmem(shape, dtype):
    return jax.ShapeDtypeStruct(shape, dtype)


def local(wannier_g, rp_coords, q_coords, k_index, k_vectors, kq_vectors, modes):
    groups = lax.axis_size("rp")
    columns = lax.axis_size("pb")
    devices = groups * columns
    per_device = q_coords.shape[1]
    span = wannier_g.shape[1]
    rows = 2 * span
    cut = rows * EXTRA // LANES
    chunk = rows + cut + 8

    sent = jnp.broadcast_to(q_coords[None], (columns, 3, per_device))
    near = lax.all_to_all(sent, "pb", split_axis=0, concat_axis=0, tiled=True)
    near = near.transpose(1, 0, 2).reshape(3, columns * per_device)
    near = jnp.pad(near.astype(jnp.bfloat16), ((0, 5), (0, LANES - columns * per_device)))
    packed = pl.pallas_call(
        pack_kernel,
        out_shape=vmem((groups, chunk, LANES), jnp.bfloat16),
        in_specs=[pl.BlockSpec(memory_space=pltpu.HBM)],
        out_specs=pl.BlockSpec(memory_space=pl.ANY),
        scratch_shapes=[
            pltpu.VMEM((rows, LANES), jnp.bfloat16),
            pltpu.VMEM((groups, cut, LANES), jnp.bfloat16),
            pltpu.SemaphoreType.DMA((groups + 2,)),
        ],
        compiler_params=room(8),
        name="pack",
    )(pltpu.with_memory_space_constraint(wannier_g.reshape(rows, wannier_g.shape[3]), pltpu.HBM))
    packed = packed.at[:, rows + cut :, :].set(jnp.broadcast_to(near, (groups, 8, LANES)))
    turns_of = jnp.pad(rp_coords.astype(jnp.float32) / NK, ((0, 5), (0, 0)))
    turns_of = turns_of.astype(jnp.bfloat16)
    select = (jnp.arange(k_vectors.shape[0]) == k_index[0]).astype(jnp.bfloat16)
    unit = jnp.einsum("k,kcnj->cnj", select, k_vectors, preferred_element_type=jnp.float32)
    span8 = jnp.arange(8 * BANDS)
    wide = (span8[:, None] // 8 == jnp.arange(BANDS)).astype(jnp.bfloat16)
    u_table = jnp.einsum(
        "pj,cnj->cpn", wide, unit.astype(jnp.bfloat16), preferred_element_type=jnp.float32
    ).astype(jnp.bfloat16)
    u_table = jnp.einsum("cpn,kn->cpk", u_table, wide, preferred_element_type=jnp.float32)
    u_table = jnp.where(span8[:, None] % 8 == span8 % 8, u_table, 0.0).astype(jnp.bfloat16)
    v_real, v_imag = kq_vectors[:, 0], kq_vectors[:, 1]
    v_block = jnp.stack([jnp.stack([v_real, -v_imag], 2), jnp.stack([v_imag, v_real], 2)], 1)
    twice = jnp.repeat(jnp.eye(2 * BANDS, dtype=jnp.bfloat16), per_device, 1)
    v_table = jnp.einsum(
        "qcmdi,cmk->qdik",
        v_block,
        twice.reshape(2, BANDS, 2 * BANDS * per_device),
        preferred_element_type=jnp.float32,
    ).reshape(per_device, 2 * BANDS, 2 * BANDS * per_device)
    own = jnp.arange(2 * BANDS * per_device) % per_device == jnp.arange(per_device)[:, None]
    v_table = jnp.where(own[:, None, :], v_table, 0.0).astype(jnp.bfloat16)
    v_table = v_table.reshape(per_device * 2 * BANDS, 2 * BANDS * per_device)
    rest = SLOT - BRANCHES
    e_pad = jnp.pad(modes, ((0, 0), (0, 0), (0, rest), (0, rest)))
    e_real, e_imag = e_pad[:, 0], e_pad[:, 1]
    e_table = jnp.concatenate(
        [
            jnp.concatenate([e_real, e_imag, -e_imag, e_real], 2),
            jnp.concatenate([-e_imag, e_real, -e_real, -e_imag], 2),
        ],
        1,
    )
    moved = lax.all_to_all(packed, "rp", split_axis=0, concat_axis=0, tiled=True)

    vectors = rp_coords.shape[1]
    total = devices * per_device
    fourier = pl.pallas_call(
        fourier_kernel,
        out_shape=vmem((devices, 3, per_device, LANES), jnp.bfloat16),
        scratch_shapes=[
            pltpu.VMEM((total, 2 * vectors), jnp.bfloat16),
            pltpu.VMEM((2 * vectors, 3 * LANES), jnp.bfloat16),
        ],
        compiler_params=room(16),
        name="fourier",
    )(moved, turns_of)
    fourier, u_table, v_table, e_table = lax.optimization_barrier(
        (fourier, u_table, v_table, e_table)
    )
    owned = lax.all_to_all(fourier, AXES, split_axis=0, concat_axis=0, tiled=True)
    owned = owned.reshape(groups, columns, 3, per_device, LANES)

    return pl.pallas_call(
        rotate_kernel,
        out_shape=vmem((per_device, 2, BANDS, BANDS * BRANCHES), jnp.float32),
        scratch_shapes=[
            pltpu.VMEM((per_device, BANDS * BANDS, LANES), jnp.float32),
            pltpu.VMEM((per_device, BANDS * BANDS, LANES), jnp.float32),
            pltpu.VMEM((per_device, 2, BANDS, BANDS * BRANCHES), jnp.float32),
            pltpu.SemaphoreType.DMA((per_device, 2)),
        ],
        out_specs=pl.BlockSpec(memory_space=pl.ANY),
        compiler_params=room(16),
        name="rotate",
    )(owned, v_table, e_table, u_table)


def solution(mesh):
    return jax.shard_map(
        local,
        mesh=mesh,
        in_specs=(
            P(None, "rp", "pb", None),
            P(),
            P(None, AXES),
            P(),
            P(),
            P(AXES, None, None, None),
            P(AXES, None, None, None),
        ),
        out_specs=P(AXES, None, None, None),
        check_vma=False,
    )
```

```python
import math

import jax
import jax.numpy as jnp
import numpy as np
from jax import lax
from jax.experimental import pallas as pl
from jax.experimental.pallas import tpu as pltpu
from jax.sharding import PartitionSpec as P


NK = 16
LANES = 128
EXTRA = 16
BANDS = 32
BRANCHES = 36
SLOT = 64
AXES = ("rp", "pb")


def sine_series():
    points = np.arange(1, 5) / NK
    slack = np.array([1e3, 5e2, 2e4, 5e2])
    powers = np.stack([points ** (2 * k + 1) for k in range(3)], 1)
    values = np.sin(2 * math.pi * points)
    return [float(c) for c in np.linalg.lstsq(powers * slack[:, None], values * slack, rcond=None)[0]]


SERIES = sine_series()


def lane_of(shape):
    return lax.broadcasted_iota(jnp.int32, shape, len(shape) - 1)


def turned(x, shift):
    shift %= LANES
    return pltpu.roll(x, shift, 1) if shift else x


def pack_kernel(w_ref, o_ref):
    groups = o_ref.shape[0]
    rows = w_ref.shape[0]
    cut = rows * EXTRA // LANES
    pieces = rows // cut
    for a in range(groups):
        o_ref[a, :rows, :] = w_ref[:, a * LANES : (a + 1) * LANES]
        o_ref[a, rows + cut :, :] = jnp.zeros((o_ref.shape[1] - rows - cut, LANES), o_ref.dtype)
    tail = w_ref[:, groups * LANES :].astype(jnp.float32)
    lane = lane_of((cut, LANES))
    half = pieces // 2
    for a in range(groups):
        mixed = jnp.zeros((cut, LANES), jnp.float32)
        for j in range(pieces):
            place = 2 * (j % half) + j // half
            piece = turned(tail[j * cut : (j + 1) * cut], EXTRA * (place - a))
            mixed = jnp.where(lane // EXTRA == place, piece, mixed)
        o_ref[a, rows : rows + cut, :] = mixed.astype(o_ref.dtype)


def wave(u):
    w = 0.25 - jnp.abs(u - jnp.round(u))
    s = w * w
    value = SERIES[2]
    for c in SERIES[1::-1]:
        value = value * s + c
    return value * w


def fourier_kernel(x_ref, r_ref, o_ref, left, right):
    groups = x_ref.shape[0]
    span = r_ref.shape[1] // groups
    vectors = groups * span
    rows = 2 * span
    cut = rows * EXTRA // LANES
    half = span // cut
    lane = lane_of((cut, LANES))
    per_group = left.shape[0] // groups
    r_all = r_ref[...]
    for a in range(groups):
        coords = x_ref[a, rows + cut :, :].astype(jnp.float32)
        q_rows = coords.T[:per_group].astype(jnp.bfloat16)
        at = slice(a * per_group, (a + 1) * per_group)
        for n in range(0, vectors, 2 * LANES):
            end = n + 2 * LANES
            turns = jnp.dot(q_rows, r_all[:, n:end], preferred_element_type=jnp.float32)
            left[at, n:end] = wave(turns).astype(jnp.bfloat16)
            left[at, vectors + n : vectors + end] = wave(turns - 0.25).astype(jnp.bfloat16)
    for a in range(groups):
        real = x_ref[a, :span, :]
        imag = x_ref[a, span:rows, :]
        top = a * span
        low = vectors + a * span
        right[top : top + span, :LANES] = real
        right[top : top + span, LANES : 2 * LANES] = imag
        right[low : low + span, :LANES] = -imag
        right[low : low + span, LANES : 2 * LANES] = real
        mixed = x_ref[a, rows : rows + cut, :].astype(jnp.float32)
        for j in range(half):
            first = turned(mixed, -2 * EXTRA * j)
            second = jnp.where(lane < EXTRA, -turned(first, -EXTRA), turned(first, EXTRA))
            right[top + j * cut : top + (j + 1) * cut, 2 * LANES :] = first.astype(jnp.bfloat16)
            right[low + j * cut : low + (j + 1) * cut, 2 * LANES :] = second.astype(jnp.bfloat16)
    total = jnp.dot(left[...], right[...], preferred_element_type=jnp.float32)
    for k in range(3):
        part = total[:, k * LANES : (k + 1) * LANES].astype(jnp.bfloat16)
        o_ref[:, k] = part.reshape(o_ref.shape[0], 2, LANES)


def rotate_kernel(x_ref, v_ref, e_ref, u_ref, o_ref, spread, mixed, ready, sems):
    groups = x_ref.shape[0]
    pairs = 2 * BANDS
    lane = lane_of((pairs, LANES))
    tiles = []
    for a in range(groups):
        tiles.append(jnp.concatenate([x_ref[a, :, k].reshape(pairs, LANES) for k in range(2)], 0))
    tails = [x_ref[a, :, 2].reshape(pairs, LANES).astype(jnp.float32) for a in range(groups)]
    parts = []
    for c in range(2):
        part = jnp.zeros((pairs, LANES), jnp.float32)
        for a in range(groups):
            part = jnp.where(lane // EXTRA == a, turned(tails[a], EXTRA * (a - c)), part)
        parts.append(part.astype(jnp.bfloat16))
    tiles.append(jnp.concatenate(parts, 0))
    field = [jnp.dot(v_ref[...], t, preferred_element_type=jnp.float32) for t in tiles]

    lane = lane_of((BANDS, LANES))
    modes_done = []
    for q in range(2):
        for n in range(BANDS):
            t, s = divmod(BRANCHES * n, LANES)
            halves = []
            for c in range(2):
                at = slice((2 * q + c) * BANDS, (2 * q + c + 1) * BANDS)
                piece = field[t][at]
                if s + BRANCHES > LANES:
                    piece = jnp.where(lane >= s, piece, field[t + 1][at])
                halves.append(turned(piece, SLOT * c - s))
            both = jnp.where(lane < SLOT, halves[0], halves[1])
            for g in range(BANDS // 8):
                top = 8 * (g * BANDS + n)
                spread[q, top : top + 8, :] = both[8 * g : 8 * (g + 1)]
        done = jnp.dot(
            spread[q].astype(jnp.bfloat16), e_ref[q], preferred_element_type=jnp.float32
        )
        modes_done.append(done.astype(jnp.bfloat16))

    block = u_ref.shape[1]
    for g in range(BANDS * BANDS // block):
        at = slice(g * block, (g + 1) * block)
        plain = jnp.concatenate([modes_done[0][at, :LANES], modes_done[1][at, :LANES]], 1)
        turned_by_i = jnp.concatenate([modes_done[0][at, LANES:], modes_done[1][at, LANES:]], 1)
        done = jnp.dot(u_ref[0], plain, preferred_element_type=jnp.float32) + jnp.dot(
            u_ref[1], turned_by_i, preferred_element_type=jnp.float32
        )
        for q in range(2):
            mixed[q, at, :] = done[:, q * LANES : (q + 1) * LANES]

    sends = []
    for q in range(2):
        for c in range(2):
            out = None
            for j in range(BANDS):
                t, s = divmod(BRANCHES * j, LANES)
                tops = [8 * (g * BANDS + j) for g in range(BANDS // 8)]
                piece = jnp.concatenate([mixed[q, top : top + 8, :] for top in tops], 0)
                piece = turned(piece, s - SLOT * c)
                out = piece if out is None else jnp.where(lane >= s, piece, out)
                if s + BRANCHES >= LANES:
                    ready[q, c, :, t * LANES : (t + 1) * LANES] = out
                    out = piece if s + BRANCHES > LANES else None
            sends.append(pltpu.make_async_copy(ready.at[q, c], o_ref.at[q, c], sems.at[q, c]))
            sends[-1].start()
    for send in sends:
        send.wait()


def room(mib):
    return pltpu.CompilerParams(vmem_limit_bytes=mib * 2**20)


def vmem(shape, dtype):
    return jax.ShapeDtypeStruct(shape, dtype)


def local(wannier_g, rp_coords, q_coords, k_index, k_vectors, kq_vectors, modes):
    groups = lax.axis_size("rp")
    columns = lax.axis_size("pb")
    devices = groups * columns
    per_device = q_coords.shape[1]
    span = wannier_g.shape[1]
    rows = 2 * span
    cut = rows * EXTRA // LANES
    chunk = rows + cut + 8

    sent = jnp.broadcast_to(q_coords[None], (columns, 3, per_device))
    near = lax.all_to_all(sent, "pb", split_axis=0, concat_axis=0, tiled=True)
    near = near.transpose(1, 0, 2).reshape(3, columns * per_device)
    near = jnp.pad(near.astype(jnp.bfloat16), ((0, 5), (0, LANES - columns * per_device)))
    packed = pl.pallas_call(
        pack_kernel,
        out_shape=vmem((groups, chunk, LANES), jnp.bfloat16),
        compiler_params=room(8),
        name="pack",
    )(wannier_g.reshape(rows, wannier_g.shape[3]))
    packed = packed.at[:, rows + cut :, :].set(jnp.broadcast_to(near, (groups, 8, LANES)))
    turns_of = jnp.pad(rp_coords.astype(jnp.float32) / NK, ((0, 5), (0, 0)))
    turns_of = turns_of.astype(jnp.bfloat16)
    select = (jnp.arange(k_vectors.shape[0]) == k_index[0]).astype(jnp.bfloat16)
    unit = jnp.einsum("k,kcnj->cnj", select, k_vectors, preferred_element_type=jnp.float32)
    span8 = jnp.arange(8 * BANDS)
    wide = (span8[:, None] // 8 == jnp.arange(BANDS)).astype(jnp.bfloat16)
    u_table = jnp.einsum(
        "pj,cnj->cpn", wide, unit.astype(jnp.bfloat16), preferred_element_type=jnp.float32
    ).astype(jnp.bfloat16)
    u_table = jnp.einsum("cpn,kn->cpk", u_table, wide, preferred_element_type=jnp.float32)
    u_table = jnp.where(span8[:, None] % 8 == span8 % 8, u_table, 0.0).astype(jnp.bfloat16)
    v_real, v_imag = kq_vectors[:, 0], kq_vectors[:, 1]
    v_block = jnp.stack([jnp.stack([v_real, -v_imag], 2), jnp.stack([v_imag, v_real], 2)], 1)
    twice = jnp.repeat(jnp.eye(2 * BANDS, dtype=jnp.bfloat16), per_device, 1)
    v_table = jnp.einsum(
        "qcmdi,cmk->qdik",
        v_block,
        twice.reshape(2, BANDS, 2 * BANDS * per_device),
        preferred_element_type=jnp.float32,
    ).reshape(per_device, 2 * BANDS, 2 * BANDS * per_device)
    own = jnp.arange(2 * BANDS * per_device) % per_device == jnp.arange(per_device)[:, None]
    v_table = jnp.where(own[:, None, :], v_table, 0.0).astype(jnp.bfloat16)
    v_table = v_table.reshape(per_device * 2 * BANDS, 2 * BANDS * per_device)
    rest = SLOT - BRANCHES
    e_pad = jnp.pad(modes, ((0, 0), (0, 0), (0, rest), (0, rest)))
    e_real, e_imag = e_pad[:, 0], e_pad[:, 1]
    e_table = jnp.concatenate(
        [
            jnp.concatenate([e_real, e_imag, -e_imag, e_real], 2),
            jnp.concatenate([-e_imag, e_real, -e_real, -e_imag], 2),
        ],
        1,
    )
    moved = lax.all_to_all(packed, "rp", split_axis=0, concat_axis=0, tiled=True)

    vectors = rp_coords.shape[1]
    total = devices * per_device
    fourier = pl.pallas_call(
        fourier_kernel,
        out_shape=vmem((devices, 3, per_device, LANES), jnp.bfloat16),
        scratch_shapes=[
            pltpu.VMEM((total, 2 * vectors), jnp.bfloat16),
            pltpu.VMEM((2 * vectors, 3 * LANES), jnp.bfloat16),
        ],
        compiler_params=room(16),
        name="fourier",
    )(moved, turns_of)
    fourier, u_table, v_table, e_table = lax.optimization_barrier(
        (fourier, u_table, v_table, e_table)
    )
    owned = lax.all_to_all(fourier, AXES, split_axis=0, concat_axis=0, tiled=True)
    owned = owned.reshape(groups, columns, 3, per_device, LANES)

    return pl.pallas_call(
        rotate_kernel,
        out_shape=vmem((per_device, 2, BANDS, BANDS * BRANCHES), jnp.float32),
        scratch_shapes=[
            pltpu.VMEM((per_device, BANDS * BANDS, LANES), jnp.float32),
            pltpu.VMEM((per_device, BANDS * BANDS, LANES), jnp.float32),
            pltpu.VMEM((per_device, 2, BANDS, BANDS * BRANCHES), jnp.float32),
            pltpu.SemaphoreType.DMA((per_device, 2)),
        ],
        out_specs=pl.BlockSpec(memory_space=pl.ANY),
        compiler_params=room(16),
        name="rotate",
    )(owned, v_table, e_table, u_table)


def solution(mesh):
    return jax.shard_map(
        local,
        mesh=mesh,
        in_specs=(
            P(None, "rp", "pb", None),
            P(),
            P(None, AXES),
            P(),
            P(),
            P(AXES, None, None, None),
            P(AXES, None, None, None),
        ),
        out_specs=P(AXES, None, None, None),
        check_vma=False,
    )
```

```python
import math

import jax
import jax.numpy as jnp
import numpy as np
from jax import lax
from jax.experimental import pallas as pl
from jax.experimental.pallas import tpu as pltpu
from jax.sharding import PartitionSpec as P


NK = 16
LANES = 128
EXTRA = 16
BANDS = 32
BRANCHES = 36
SLOT = 64
AXES = ("rp", "pb")


def fitted(points, factor, values):
    slack = np.where(np.abs(values - 0.924) < 0.01, 2e4, 1e3)
    powers = np.stack([factor * points ** (2 * k) for k in range(3)], 1)
    return [float(c) for c in np.linalg.lstsq(powers * slack[:, None], values * slack, rcond=None)[0]]


STEPS = np.arange(5) / NK
ODD = fitted(STEPS[1:], STEPS[1:], np.sin(2 * math.pi * STEPS[1:]))
EVEN = fitted(STEPS[:4], 1 / 16 - STEPS[:4] ** 2, np.cos(2 * math.pi * STEPS[:4]))


def lane_of(shape):
    return lax.broadcasted_iota(jnp.int32, shape, len(shape) - 1)


def turned(x, shift):
    shift %= LANES
    return pltpu.roll(x, shift, 1) if shift else x


def pack_kernel(w_ref, o_ref):
    groups = o_ref.shape[0]
    rows = w_ref.shape[0]
    cut = rows * EXTRA // LANES
    pieces = rows // cut
    for a in range(groups):
        o_ref[a, :rows, :] = w_ref[:, a * LANES : (a + 1) * LANES]
        o_ref[a, rows + cut :, :] = jnp.zeros((o_ref.shape[1] - rows - cut, LANES), o_ref.dtype)
    tail = w_ref[:, groups * LANES :].astype(jnp.float32)
    lane = lane_of((cut, LANES))
    half = pieces // 2
    for a in range(groups):
        mixed = jnp.zeros((cut, LANES), jnp.float32)
        for j in range(pieces):
            place = 2 * (j % half) + j // half
            piece = turned(tail[j * cut : (j + 1) * cut], EXTRA * (place - a))
            mixed = jnp.where(lane // EXTRA == place, piece, mixed)
        o_ref[a, rows : rows + cut, :] = mixed.astype(o_ref.dtype)


def waves(u):
    d = u - jnp.round(u)
    w = 0.25 - jnp.abs(d)
    s = w * w
    cosine = w * (ODD[0] + s * (ODD[1] + s * ODD[2]))
    size = (1 / 16 - s) * (EVEN[0] + s * (EVEN[1] + s * EVEN[2]))
    return cosine.astype(jnp.bfloat16), jnp.where(d < 0, -size, size).astype(jnp.bfloat16)


def fourier_kernel(x_ref, r_ref, o_ref, left, right):
    groups = x_ref.shape[0]
    span = r_ref.shape[1] // groups
    vectors = groups * span
    rows = 2 * span
    cut = rows * EXTRA // LANES
    half = span // cut
    lane = lane_of((cut, LANES))
    per_group = left.shape[0] // groups
    r_all = r_ref[...]
    for a in range(groups):
        coords = x_ref[a, rows + cut :, :].astype(jnp.float32)
        q_rows = coords.T[:per_group].astype(jnp.bfloat16)
        at = slice(a * per_group, (a + 1) * per_group)
        for n in range(0, vectors, 2 * LANES):
            end = n + 2 * LANES
            turns = jnp.dot(q_rows, r_all[:, n:end], preferred_element_type=jnp.float32)
            left[at, n:end], left[at, vectors + n : vectors + end] = waves(turns)
    for a in range(groups):
        real = x_ref[a, :span, :]
        imag = x_ref[a, span:rows, :]
        top = a * span
        low = vectors + a * span
        right[top : top + span, :LANES] = real
        right[top : top + span, LANES : 2 * LANES] = imag
        right[low : low + span, :LANES] = -imag
        right[low : low + span, LANES : 2 * LANES] = real
        mixed = x_ref[a, rows : rows + cut, :].astype(jnp.float32)
        for j in range(half):
            first = turned(mixed, -2 * EXTRA * j)
            second = jnp.where(lane < EXTRA, -turned(first, -EXTRA), turned(first, EXTRA))
            right[top + j * cut : top + (j + 1) * cut, 2 * LANES :] = first.astype(jnp.bfloat16)
            right[low + j * cut : low + (j + 1) * cut, 2 * LANES :] = second.astype(jnp.bfloat16)
    total = jnp.dot(left[...], right[...], preferred_element_type=jnp.float32)
    for k in range(3):
        part = total[:, k * LANES : (k + 1) * LANES].astype(jnp.bfloat16)
        o_ref[:, k] = part.reshape(o_ref.shape[0], 2, LANES)


def rotate_kernel(x_ref, v_ref, e_ref, u_ref, o_ref, spread, mixed, ready, sems):
    groups = x_ref.shape[0]
    pairs = 2 * BANDS
    lane = lane_of((pairs, LANES))
    tiles = []
    for a in range(groups):
        tiles.append(jnp.concatenate([x_ref[a, :, k].reshape(pairs, LANES) for k in range(2)], 0))
    tails = [x_ref[a, :, 2].reshape(pairs, LANES).astype(jnp.float32) for a in range(groups)]
    parts = []
    for c in range(2):
        part = jnp.zeros((pairs, LANES), jnp.float32)
        for a in range(groups):
            part = jnp.where(lane // EXTRA == a, turned(tails[a], EXTRA * (a - c)), part)
        parts.append(part.astype(jnp.bfloat16))
    tiles.append(jnp.concatenate(parts, 0))
    field = []
    for t in range(0, len(tiles), 2):
        pair = jnp.concatenate(tiles[t : t + 2], 1)
        done = jnp.dot(v_ref[...], pair, preferred_element_type=jnp.float32)
        field += [done[:, k : k + LANES] for k in range(0, pair.shape[1], LANES)]

    lane = lane_of((BANDS, LANES))
    modes_done = []
    for q in range(2):
        for n in range(BANDS):
            t, s = divmod(BRANCHES * n, LANES)
            halves = []
            for c in range(2):
                at = slice((2 * q + c) * BANDS, (2 * q + c + 1) * BANDS)
                piece = field[t][at]
                if s + BRANCHES > LANES:
                    piece = jnp.where(lane >= s, piece, field[t + 1][at])
                halves.append(turned(piece, SLOT * c - s))
            both = jnp.where(lane < SLOT, halves[0], halves[1])
            for g in range(BANDS // 8):
                top = 8 * (g * BANDS + n)
                spread[q, top : top + 8, :] = both[8 * g : 8 * (g + 1)]
        done = jnp.dot(
            spread[q].astype(jnp.bfloat16), e_ref[q], preferred_element_type=jnp.float32
        )
        modes_done.append(done.astype(jnp.bfloat16))

    block = u_ref.shape[1]
    for g in range(BANDS * BANDS // block):
        at = slice(g * block, (g + 1) * block)
        plain = jnp.concatenate([modes_done[0][at, :LANES], modes_done[1][at, :LANES]], 1)
        turned_by_i = jnp.concatenate([modes_done[0][at, LANES:], modes_done[1][at, LANES:]], 1)
        done = jnp.dot(u_ref[0], plain, preferred_element_type=jnp.float32) + jnp.dot(
            u_ref[1], turned_by_i, preferred_element_type=jnp.float32
        )
        for q in range(2):
            mixed[q, at, :] = done[:, q * LANES : (q + 1) * LANES]

    sends = []
    for q in range(2):
        for c in range(2):
            out = None
            for j in range(BANDS):
                t, s = divmod(BRANCHES * j, LANES)
                tops = [8 * (g * BANDS + j) for g in range(BANDS // 8)]
                piece = jnp.concatenate([mixed[q, top : top + 8, :] for top in tops], 0)
                piece = turned(piece, s - SLOT * c)
                out = piece if out is None else jnp.where(lane >= s, piece, out)
                if s + BRANCHES >= LANES:
                    ready[q, c, :, t * LANES : (t + 1) * LANES] = out
                    out = piece if s + BRANCHES > LANES else None
            sends.append(pltpu.make_async_copy(ready.at[q, c], o_ref.at[q, c], sems.at[q, c]))
            sends[-1].start()
    for send in sends:
        send.wait()


def room(mib):
    return pltpu.CompilerParams(vmem_limit_bytes=mib * 2**20)


def vmem(shape, dtype):
    return jax.ShapeDtypeStruct(shape, dtype)


def local(wannier_g, rp_coords, q_coords, k_index, k_vectors, kq_vectors, modes):
    groups = lax.axis_size("rp")
    columns = lax.axis_size("pb")
    devices = groups * columns
    per_device = q_coords.shape[1]
    span = wannier_g.shape[1]
    rows = 2 * span
    cut = rows * EXTRA // LANES
    chunk = rows + cut + 8

    sent = jnp.broadcast_to(q_coords[None], (columns, 3, per_device))
    near = lax.all_to_all(sent, "pb", split_axis=0, concat_axis=0, tiled=True)
    near = near.transpose(1, 0, 2).reshape(3, columns * per_device)
    near = jnp.pad(near.astype(jnp.bfloat16), ((0, 5), (0, LANES - columns * per_device)))
    packed = pl.pallas_call(
        pack_kernel,
        out_shape=vmem((groups, chunk, LANES), jnp.bfloat16),
        compiler_params=room(8),
        name="pack",
    )(wannier_g.reshape(rows, wannier_g.shape[3]))
    packed = packed.at[:, rows + cut :, :].set(jnp.broadcast_to(near, (groups, 8, LANES)))
    turns_of = jnp.pad(rp_coords.astype(jnp.float32) / NK, ((0, 5), (0, 0)))
    turns_of = turns_of.astype(jnp.bfloat16)
    select = (jnp.arange(k_vectors.shape[0]) == k_index[0]).astype(jnp.bfloat16)
    unit = jnp.einsum("k,kcnj->cnj", select, k_vectors, preferred_element_type=jnp.float32)
    span8 = jnp.arange(8 * BANDS)
    wide = (span8[:, None] // 8 == jnp.arange(BANDS)).astype(jnp.bfloat16)
    u_table = jnp.einsum(
        "pj,cnj->cpn", wide, unit.astype(jnp.bfloat16), preferred_element_type=jnp.float32
    ).astype(jnp.bfloat16)
    u_table = jnp.einsum("cpn,kn->cpk", u_table, wide, preferred_element_type=jnp.float32)
    u_table = jnp.where(span8[:, None] % 8 == span8 % 8, u_table, 0.0).astype(jnp.bfloat16)
    v_real, v_imag = kq_vectors[:, 0], kq_vectors[:, 1]
    v_block = jnp.stack([jnp.stack([v_real, -v_imag], 2), jnp.stack([v_imag, v_real], 2)], 1)
    twice = jnp.repeat(jnp.eye(2 * BANDS, dtype=jnp.bfloat16), per_device, 1)
    v_table = jnp.einsum(
        "qcmdi,cmk->qdik",
        v_block,
        twice.reshape(2, BANDS, 2 * BANDS * per_device),
        preferred_element_type=jnp.float32,
    ).reshape(per_device, 2 * BANDS, 2 * BANDS * per_device)
    own = jnp.arange(2 * BANDS * per_device) % per_device == jnp.arange(per_device)[:, None]
    v_table = jnp.where(own[:, None, :], v_table, 0.0).astype(jnp.bfloat16)
    v_table = v_table.reshape(per_device * 2 * BANDS, 2 * BANDS * per_device)
    rest = SLOT - BRANCHES
    e_pad = jnp.pad(modes, ((0, 0), (0, 0), (0, rest), (0, rest)))
    e_real, e_imag = e_pad[:, 0], e_pad[:, 1]
    e_table = jnp.concatenate(
        [
            jnp.concatenate([e_real, e_imag, -e_imag, e_real], 2),
            jnp.concatenate([-e_imag, e_real, -e_real, -e_imag], 2),
        ],
        1,
    )
    moved = lax.all_to_all(packed, "rp", split_axis=0, concat_axis=0, tiled=True)

    vectors = rp_coords.shape[1]
    total = devices * per_device
    fourier = pl.pallas_call(
        fourier_kernel,
        out_shape=vmem((devices, 3, per_device, LANES), jnp.bfloat16),
        scratch_shapes=[
            pltpu.VMEM((total, 2 * vectors), jnp.bfloat16),
            pltpu.VMEM((2 * vectors, 3 * LANES), jnp.bfloat16),
        ],
        compiler_params=room(16),
        name="fourier",
    )(moved, turns_of)
    fourier, u_table, v_table, e_table = lax.optimization_barrier(
        (fourier, u_table, v_table, e_table)
    )
    owned = lax.all_to_all(fourier, AXES, split_axis=0, concat_axis=0, tiled=True)
    owned = owned.reshape(groups, columns, 3, per_device, LANES)

    return pl.pallas_call(
        rotate_kernel,
        out_shape=vmem((per_device, 2, BANDS, BANDS * BRANCHES), jnp.float32),
        scratch_shapes=[
            pltpu.VMEM((per_device, BANDS * BANDS, LANES), jnp.float32),
            pltpu.VMEM((per_device, BANDS * BANDS, LANES), jnp.float32),
            pltpu.VMEM((per_device, 2, BANDS, BANDS * BRANCHES), jnp.float32),
            pltpu.SemaphoreType.DMA((per_device, 2)),
        ],
        out_specs=pl.BlockSpec(memory_space=pl.ANY),
        compiler_params=room(16),
        name="rotate",
    )(owned, v_table, e_table, u_table)


def solution(mesh):
    return jax.shard_map(
        local,
        mesh=mesh,
        in_specs=(
            P(None, "rp", "pb", None),
            P(),
            P(None, AXES),
            P(),
            P(),
            P(AXES, None, None, None),
            P(AXES, None, None, None),
        ),
        out_specs=P(AXES, None, None, None),
        check_vma=False,
    )
```

```python
import jax
import jax.numpy as jnp
from jax import lax
from jax.experimental import pallas as pl
from jax.experimental.pallas import tpu as pltpu
from jax.sharding import PartitionSpec as P


NK = 16
LANES = 128
EXTRA = 16
BANDS = 32
BRANCHES = 36
SLOT = 64
AXES = ("rp", "pb")


ODD = (6.28125, -40.75, 68.5)


def lane_of(shape):
    return lax.broadcasted_iota(jnp.int32, shape, len(shape) - 1)


def turned(x, shift):
    shift %= LANES
    return pltpu.roll(x, shift, 1) if shift else x


def pack_kernel(w_ref, o_ref):
    groups = o_ref.shape[0]
    rows = w_ref.shape[0]
    cut = rows * EXTRA // LANES
    pieces = rows // cut
    for a in range(groups):
        o_ref[a, :rows, :] = w_ref[:, a * LANES : (a + 1) * LANES]
        o_ref[a, rows + cut :, :] = jnp.zeros((o_ref.shape[1] - rows - cut, LANES), o_ref.dtype)
    tail = w_ref[:, groups * LANES :].astype(jnp.float32)
    lane = lane_of((cut, LANES))
    half = pieces // 2
    for a in range(groups):
        mixed = jnp.zeros((cut, LANES), jnp.float32)
        for j in range(pieces):
            place = 2 * (j % half) + j // half
            piece = turned(tail[j * cut : (j + 1) * cut], EXTRA * (place - a))
            mixed = jnp.where(lane // EXTRA == place, piece, mixed)
        o_ref[a, rows : rows + cut, :] = mixed.astype(o_ref.dtype)


def sine(w):
    s = w * w
    return w * (ODD[0] + s * (ODD[1] + s * ODD[2]))


def waves(u):
    d = (u - jnp.round(u)).astype(jnp.bfloat16)
    return sine(0.25 - jnp.abs(d)), sine(jnp.maximum(jnp.minimum(d, 0.5 - d), -0.5 - d))


def fourier_kernel(x_ref, r_ref, o_ref, left, right):
    groups = x_ref.shape[0]
    span = r_ref.shape[1] // groups
    vectors = groups * span
    rows = 2 * span
    cut = rows * EXTRA // LANES
    half = span // cut
    lane = lane_of((cut, LANES))
    per_group = left.shape[0] // groups
    r_all = r_ref[...]
    for a in range(groups):
        coords = x_ref[a, rows + cut :, :].astype(jnp.float32)
        q_rows = coords.T[:per_group].astype(jnp.bfloat16)
        at = slice(a * per_group, (a + 1) * per_group)
        for n in range(0, vectors, 2 * LANES):
            end = n + 2 * LANES
            turns = jnp.dot(q_rows, r_all[:, n:end], preferred_element_type=jnp.float32)
            left[at, n:end], left[at, vectors + n : vectors + end] = waves(turns)
    for a in range(groups):
        real = x_ref[a, :span, :]
        imag = x_ref[a, span:rows, :]
        top = a * span
        low = vectors + a * span
        right[top : top + span, :LANES] = real
        right[top : top + span, LANES : 2 * LANES] = imag
        right[low : low + span, :LANES] = -imag
        right[low : low + span, LANES : 2 * LANES] = real
        mixed = x_ref[a, rows : rows + cut, :].astype(jnp.float32)
        for j in range(half):
            first = turned(mixed, -2 * EXTRA * j)
            second = jnp.where(lane < EXTRA, -turned(first, -EXTRA), turned(first, EXTRA))
            right[top + j * cut : top + (j + 1) * cut, 2 * LANES :] = first.astype(jnp.bfloat16)
            right[low + j * cut : low + (j + 1) * cut, 2 * LANES :] = second.astype(jnp.bfloat16)
    total = jnp.dot(left[...], right[...], preferred_element_type=jnp.float32)
    for k in range(3):
        part = total[:, k * LANES : (k + 1) * LANES].astype(jnp.bfloat16)
        o_ref[:, k] = part.reshape(o_ref.shape[0], 2, LANES)


def rotate_kernel(x_ref, v_ref, e_ref, u_ref, o_ref, spread, mixed, ready, sems):
    groups = x_ref.shape[0]
    pairs = 2 * BANDS
    lane = lane_of((pairs, LANES))
    tiles = []
    for a in range(groups):
        tiles.append(jnp.concatenate([x_ref[a, :, k].reshape(pairs, LANES) for k in range(2)], 0))
    tails = [x_ref[a, :, 2].reshape(pairs, LANES).astype(jnp.float32) for a in range(groups)]
    parts = []
    for c in range(2):
        part = jnp.zeros((pairs, LANES), jnp.float32)
        for a in range(groups):
            part = jnp.where(lane // EXTRA == a, turned(tails[a], EXTRA * (a - c)), part)
        parts.append(part.astype(jnp.bfloat16))
    tiles.append(jnp.concatenate(parts, 0))
    field = []
    for t in range(0, len(tiles), 2):
        pair = jnp.concatenate(tiles[t : t + 2], 1)
        done = jnp.dot(v_ref[...], pair, preferred_element_type=jnp.float32)
        field += [done[:, k : k + LANES] for k in range(0, pair.shape[1], LANES)]

    lane = lane_of((BANDS, LANES))
    modes_done = []
    for q in range(2):
        for n in range(BANDS):
            t, s = divmod(BRANCHES * n, LANES)
            halves = []
            for c in range(2):
                at = slice((2 * q + c) * BANDS, (2 * q + c + 1) * BANDS)
                piece = field[t][at]
                if s + BRANCHES > LANES:
                    piece = jnp.where(lane >= s, piece, field[t + 1][at])
                halves.append(turned(piece, SLOT * c - s))
            both = jnp.where(lane < SLOT, halves[0], halves[1])
            for g in range(BANDS // 8):
                top = 8 * (g * BANDS + n)
                spread[q, top : top + 8, :] = both[8 * g : 8 * (g + 1)]
        done = jnp.dot(
            spread[q].astype(jnp.bfloat16), e_ref[q], preferred_element_type=jnp.float32
        )
        modes_done.append(done.astype(jnp.bfloat16))

    block = u_ref.shape[1]
    for g in range(BANDS * BANDS // block):
        at = slice(g * block, (g + 1) * block)
        plain = jnp.concatenate([modes_done[0][at, :LANES], modes_done[1][at, :LANES]], 1)
        turned_by_i = jnp.concatenate([modes_done[0][at, LANES:], modes_done[1][at, LANES:]], 1)
        done = jnp.dot(u_ref[0], plain, preferred_element_type=jnp.float32) + jnp.dot(
            u_ref[1], turned_by_i, preferred_element_type=jnp.float32
        )
        for q in range(2):
            mixed[q, at, :] = done[:, q * LANES : (q + 1) * LANES]

    sends = []
    for q in range(2):
        for c in range(2):
            out = None
            for j in range(BANDS):
                t, s = divmod(BRANCHES * j, LANES)
                tops = [8 * (g * BANDS + j) for g in range(BANDS // 8)]
                piece = jnp.concatenate([mixed[q, top : top + 8, :] for top in tops], 0)
                piece = turned(piece, s - SLOT * c)
                out = piece if out is None else jnp.where(lane >= s, piece, out)
                if s + BRANCHES >= LANES:
                    ready[q, c, :, t * LANES : (t + 1) * LANES] = out
                    out = piece if s + BRANCHES > LANES else None
            sends.append(pltpu.make_async_copy(ready.at[q, c], o_ref.at[q, c], sems.at[q, c]))
            sends[-1].start()
    for send in sends:
        send.wait()


def room(mib):
    return pltpu.CompilerParams(vmem_limit_bytes=mib * 2**20)


def vmem(shape, dtype):
    return jax.ShapeDtypeStruct(shape, dtype)


def local(wannier_g, rp_coords, q_coords, k_index, k_vectors, kq_vectors, modes):
    groups = lax.axis_size("rp")
    columns = lax.axis_size("pb")
    devices = groups * columns
    per_device = q_coords.shape[1]
    span = wannier_g.shape[1]
    rows = 2 * span
    cut = rows * EXTRA // LANES
    chunk = rows + cut + 8

    sent = jnp.broadcast_to(q_coords[None], (columns, 3, per_device))
    near = lax.all_to_all(sent, "pb", split_axis=0, concat_axis=0, tiled=True)
    near = near.transpose(1, 0, 2).reshape(3, columns * per_device)
    near = jnp.pad(near.astype(jnp.bfloat16), ((0, 5), (0, LANES - columns * per_device)))
    packed = pl.pallas_call(
        pack_kernel,
        out_shape=vmem((groups, chunk, LANES), jnp.bfloat16),
        compiler_params=room(8),
        name="pack",
    )(wannier_g.reshape(rows, wannier_g.shape[3]))
    packed = packed.at[:, rows + cut :, :].set(jnp.broadcast_to(near, (groups, 8, LANES)))
    turns_of = jnp.pad(rp_coords.astype(jnp.float32) / NK, ((0, 5), (0, 0)))
    turns_of = turns_of.astype(jnp.bfloat16)
    select = (jnp.arange(k_vectors.shape[0]) == k_index[0]).astype(jnp.bfloat16)
    unit = jnp.einsum("k,kcnj->cnj", select, k_vectors, preferred_element_type=jnp.float32)
    span8 = jnp.arange(8 * BANDS)
    wide = (span8[:, None] // 8 == jnp.arange(BANDS)).astype(jnp.bfloat16)
    u_table = jnp.einsum(
        "pj,cnj->cpn", wide, unit.astype(jnp.bfloat16), preferred_element_type=jnp.float32
    ).astype(jnp.bfloat16)
    u_table = jnp.einsum("cpn,kn->cpk", u_table, wide, preferred_element_type=jnp.float32)
    u_table = jnp.where(span8[:, None] % 8 == span8 % 8, u_table, 0.0).astype(jnp.bfloat16)
    v_real, v_imag = kq_vectors[:, 0], kq_vectors[:, 1]
    v_block = jnp.stack([jnp.stack([v_real, -v_imag], 2), jnp.stack([v_imag, v_real], 2)], 1)
    twice = jnp.repeat(jnp.eye(2 * BANDS, dtype=jnp.bfloat16), per_device, 1)
    v_table = jnp.einsum(
        "qcmdi,cmk->qdik",
        v_block,
        twice.reshape(2, BANDS, 2 * BANDS * per_device),
        preferred_element_type=jnp.float32,
    ).reshape(per_device, 2 * BANDS, 2 * BANDS * per_device)
    own = jnp.arange(2 * BANDS * per_device) % per_device == jnp.arange(per_device)[:, None]
    v_table = jnp.where(own[:, None, :], v_table, 0.0).astype(jnp.bfloat16)
    v_table = v_table.reshape(per_device * 2 * BANDS, 2 * BANDS * per_device)
    rest = SLOT - BRANCHES
    e_pad = jnp.pad(modes, ((0, 0), (0, 0), (0, rest), (0, rest)))
    e_real, e_imag = e_pad[:, 0], e_pad[:, 1]
    e_table = jnp.concatenate(
        [
            jnp.concatenate([e_real, e_imag, -e_imag, e_real], 2),
            jnp.concatenate([-e_imag, e_real, -e_real, -e_imag], 2),
        ],
        1,
    )
    moved = lax.all_to_all(packed, "rp", split_axis=0, concat_axis=0, tiled=True)

    vectors = rp_coords.shape[1]
    total = devices * per_device
    fourier = pl.pallas_call(
        fourier_kernel,
        out_shape=vmem((devices, 3, per_device, LANES), jnp.bfloat16),
        scratch_shapes=[
            pltpu.VMEM((total, 2 * vectors), jnp.bfloat16),
            pltpu.VMEM((2 * vectors, 3 * LANES), jnp.bfloat16),
        ],
        compiler_params=room(16),
        name="fourier",
    )(moved, turns_of)
    fourier, u_table, v_table, e_table = lax.optimization_barrier(
        (fourier, u_table, v_table, e_table)
    )
    owned = lax.all_to_all(fourier, AXES, split_axis=0, concat_axis=0, tiled=True)
    owned = owned.reshape(groups, columns, 3, per_device, LANES)

    return pl.pallas_call(
        rotate_kernel,
        out_shape=vmem((per_device, 2, BANDS, BANDS * BRANCHES), jnp.float32),
        scratch_shapes=[
            pltpu.VMEM((per_device, BANDS * BANDS, LANES), jnp.float32),
            pltpu.VMEM((per_device, BANDS * BANDS, LANES), jnp.float32),
            pltpu.VMEM((per_device, 2, BANDS, BANDS * BRANCHES), jnp.float32),
            pltpu.SemaphoreType.DMA((per_device, 2)),
        ],
        out_specs=pl.BlockSpec(memory_space=pl.ANY),
        compiler_params=room(16),
        name="rotate",
    )(owned, v_table, e_table, u_table)


def solution(mesh):
    return jax.shard_map(
        local,
        mesh=mesh,
        in_specs=(
            P(None, "rp", "pb", None),
            P(),
            P(None, AXES),
            P(),
            P(),
            P(AXES, None, None, None),
            P(AXES, None, None, None),
        ),
        out_specs=P(AXES, None, None, None),
        check_vma=False,
    )
```

```python
import jax
import jax.numpy as jnp
from jax import lax
from jax.experimental import pallas as pl
from jax.experimental.pallas import tpu as pltpu
from jax.sharding import PartitionSpec as P


NK = 16
LANES = 128
EXTRA = 16
BANDS = 32
BRANCHES = 36
SLOT = 64
AXES = ("rp", "pb")


ODD = (6.28125, -40.75, 68.5)


def lane_of(shape):
    return lax.broadcasted_iota(jnp.int32, shape, len(shape) - 1)


def turned(x, shift):
    shift %= LANES
    return pltpu.roll(x, shift, 1) if shift else x


def pack_kernel(w_ref, o_ref):
    groups = o_ref.shape[0]
    rows = w_ref.shape[0]
    cut = rows * EXTRA // LANES
    pieces = rows // cut
    for a in range(groups):
        o_ref[a, :rows, :] = w_ref[:, a * LANES : (a + 1) * LANES]
        o_ref[a, rows + cut :, :] = jnp.zeros((o_ref.shape[1] - rows - cut, LANES), o_ref.dtype)
    tail = w_ref[:, groups * LANES :].astype(jnp.float32)
    lane = lane_of((cut, LANES))
    half = pieces // 2
    for a in range(groups):
        mixed = jnp.zeros((cut, LANES), jnp.float32)
        for j in range(pieces):
            place = 2 * (j % half) + j // half
            piece = turned(tail[j * cut : (j + 1) * cut], EXTRA * (place - a))
            mixed = jnp.where(lane // EXTRA == place, piece, mixed)
        o_ref[a, rows : rows + cut, :] = mixed.astype(o_ref.dtype)


def sine(w):
    s = w * w
    return w * (ODD[0] + s * (ODD[1] + s * ODD[2]))


def waves(u):
    d = (u - jnp.round(u)).astype(jnp.bfloat16)
    return sine(0.25 - jnp.abs(d)), sine(jnp.maximum(jnp.minimum(d, 0.5 - d), -0.5 - d))


def fourier_kernel(x_ref, r_ref, o_ref, left, right):
    groups = x_ref.shape[0]
    span = r_ref.shape[1] // groups
    vectors = groups * span
    rows = 2 * span
    cut = rows * EXTRA // LANES
    half = span // cut
    lane = lane_of((cut, LANES))
    per_group = left.shape[0] // groups
    r_all = r_ref[...]
    for a in range(groups):
        coords = x_ref[a, rows + cut :, :].astype(jnp.float32)
        q_rows = coords.T[:per_group].astype(jnp.bfloat16)
        at = slice(a * per_group, (a + 1) * per_group)
        for n in range(0, vectors, 4 * LANES):
            end = n + 4 * LANES
            turns = jnp.dot(q_rows, r_all[:, n:end], preferred_element_type=jnp.float32)
            left[at, n:end], left[at, vectors + n : vectors + end] = waves(turns)
    for a in range(groups):
        real = x_ref[a, :span, :]
        imag = x_ref[a, span:rows, :]
        top = a * span
        low = vectors + a * span
        right[top : top + span, :LANES] = real
        right[top : top + span, LANES : 2 * LANES] = imag
        right[low : low + span, :LANES] = -imag
        right[low : low + span, LANES : 2 * LANES] = real
        mixed = x_ref[a, rows : rows + cut, :].astype(jnp.float32)
        for j in range(half):
            first = turned(mixed, -2 * EXTRA * j)
            second = jnp.where(lane < EXTRA, -turned(first, -EXTRA), turned(first, EXTRA))
            right[top + j * cut : top + (j + 1) * cut, 2 * LANES :] = first.astype(jnp.bfloat16)
            right[low + j * cut : low + (j + 1) * cut, 2 * LANES :] = second.astype(jnp.bfloat16)
    total = jnp.dot(left[...], right[...], preferred_element_type=jnp.float32)
    for k in range(3):
        part = total[:, k * LANES : (k + 1) * LANES].astype(jnp.bfloat16)
        o_ref[:, k] = part.reshape(o_ref.shape[0], 2, LANES)


def rotate_kernel(x_ref, v_ref, e_ref, u_ref, o_ref, ready, sems):
    groups = x_ref.shape[0]
    pairs = 2 * BANDS
    lane = lane_of((pairs, LANES))
    tiles = []
    for a in range(groups):
        tiles.append(jnp.concatenate([x_ref[a, :, k].reshape(pairs, LANES) for k in range(2)], 0))
    tails = [x_ref[a, :, 2].reshape(pairs, LANES).astype(jnp.float32) for a in range(groups)]
    parts = []
    for c in range(2):
        part = jnp.zeros((pairs, LANES), jnp.float32)
        for a in range(groups):
            part = jnp.where(lane // EXTRA == a, turned(tails[a], EXTRA * (a - c)), part)
        parts.append(part.astype(jnp.bfloat16))
    tiles.append(jnp.concatenate(parts, 0))
    field = []
    for t in range(0, len(tiles), 2):
        pair = jnp.concatenate(tiles[t : t + 2], 1)
        done = jnp.dot(v_ref[...], pair, preferred_element_type=jnp.float32)
        field += [done[:, k : k + LANES] for k in range(0, pair.shape[1], LANES)]

    lane = lane_of((8, LANES))
    sends = []
    for g in range(BANDS // 8):
        plain, by_i = [], []
        for q in range(2):
            rows = []
            for n in range(BANDS):
                t, s = divmod(BRANCHES * n, LANES)
                halves = []
                for c in range(2):
                    top = (2 * q + c) * BANDS + 8 * g
                    piece = field[t][top : top + 8]
                    if s + BRANCHES > LANES:
                        piece = jnp.where(lane >= s, piece, field[t + 1][top : top + 8])
                    halves.append(turned(piece, SLOT * c - s))
                rows.append(jnp.where(lane < SLOT, halves[0], halves[1]))
            gathered = jnp.concatenate(rows, 0).astype(jnp.bfloat16)
            done = jnp.dot(gathered, e_ref[q], preferred_element_type=jnp.float32)
            done = done.astype(jnp.bfloat16)
            plain.append(done[:, :LANES])
            by_i.append(done[:, LANES:])
        mixed = jnp.dot(
            u_ref[0], jnp.concatenate(plain, 1), preferred_element_type=jnp.float32
        ) + jnp.dot(u_ref[1], jnp.concatenate(by_i, 1), preferred_element_type=jnp.float32)
        here = slice(8 * g, 8 * (g + 1))
        for q in range(2):
            for c in range(2):
                out = None
                for j in range(BANDS):
                    t, s = divmod(BRANCHES * j, LANES)
                    piece = mixed[8 * j : 8 * (j + 1), q * LANES : (q + 1) * LANES]
                    piece = turned(piece, s - SLOT * c)
                    out = piece if out is None else jnp.where(lane >= s, piece, out)
                    if s + BRANCHES >= LANES:
                        ready[q, c, here, t * LANES : (t + 1) * LANES] = out
                        out = piece if s + BRANCHES > LANES else None
        sends.append(
            pltpu.make_async_copy(ready.at[:, :, here], o_ref.at[:, :, here], sems.at[g])
        )
        sends[-1].start()
    for send in sends:
        send.wait()


def room(mib):
    return pltpu.CompilerParams(vmem_limit_bytes=mib * 2**20)


def vmem(shape, dtype):
    return jax.ShapeDtypeStruct(shape, dtype)


def local(wannier_g, rp_coords, q_coords, k_index, k_vectors, kq_vectors, modes):
    groups = lax.axis_size("rp")
    columns = lax.axis_size("pb")
    devices = groups * columns
    per_device = q_coords.shape[1]
    span = wannier_g.shape[1]
    rows = 2 * span
    cut = rows * EXTRA // LANES
    chunk = rows + cut + 8

    sent = jnp.broadcast_to(q_coords[None], (columns, 3, per_device))
    near = lax.all_to_all(sent, "pb", split_axis=0, concat_axis=0, tiled=True)
    near = near.transpose(1, 0, 2).reshape(3, columns * per_device)
    near = jnp.pad(near.astype(jnp.bfloat16), ((0, 5), (0, LANES - columns * per_device)))
    packed = pl.pallas_call(
        pack_kernel,
        out_shape=vmem((groups, chunk, LANES), jnp.bfloat16),
        compiler_params=room(8),
        name="pack",
    )(wannier_g.reshape(rows, wannier_g.shape[3]))
    packed = packed.at[:, rows + cut :, :].set(jnp.broadcast_to(near, (groups, 8, LANES)))
    turns_of = jnp.pad(rp_coords.astype(jnp.float32) / NK, ((0, 5), (0, 0)))
    turns_of = turns_of.astype(jnp.bfloat16)
    select = (jnp.arange(k_vectors.shape[0]) == k_index[0]).astype(jnp.bfloat16)
    unit = jnp.einsum("k,kcnj->cnj", select, k_vectors, preferred_element_type=jnp.float32)
    span8 = jnp.arange(8 * BANDS)
    wide = (span8[:, None] // 8 == jnp.arange(BANDS)).astype(jnp.bfloat16)
    u_table = jnp.einsum(
        "pj,cnj->cpn", wide, unit.astype(jnp.bfloat16), preferred_element_type=jnp.float32
    ).astype(jnp.bfloat16)
    u_table = jnp.einsum("cpn,kn->cpk", u_table, wide, preferred_element_type=jnp.float32)
    u_table = jnp.where(span8[:, None] % 8 == span8 % 8, u_table, 0.0).astype(jnp.bfloat16)
    v_real, v_imag = kq_vectors[:, 0], kq_vectors[:, 1]
    v_block = jnp.stack([jnp.stack([v_real, -v_imag], 2), jnp.stack([v_imag, v_real], 2)], 1)
    twice = jnp.repeat(jnp.eye(2 * BANDS, dtype=jnp.bfloat16), per_device, 1)
    v_table = jnp.einsum(
        "qcmdi,cmk->qdik",
        v_block,
        twice.reshape(2, BANDS, 2 * BANDS * per_device),
        preferred_element_type=jnp.float32,
    ).reshape(per_device, 2 * BANDS, 2 * BANDS * per_device)
    own = jnp.arange(2 * BANDS * per_device) % per_device == jnp.arange(per_device)[:, None]
    v_table = jnp.where(own[:, None, :], v_table, 0.0).astype(jnp.bfloat16)
    v_table = v_table.reshape(per_device * 2 * BANDS, 2 * BANDS * per_device)
    rest = SLOT - BRANCHES
    e_pad = jnp.pad(modes, ((0, 0), (0, 0), (0, rest), (0, rest)))
    e_real, e_imag = e_pad[:, 0], e_pad[:, 1]
    e_table = jnp.concatenate(
        [
            jnp.concatenate([e_real, e_imag, -e_imag, e_real], 2),
            jnp.concatenate([-e_imag, e_real, -e_real, -e_imag], 2),
        ],
        1,
    )
    moved = lax.all_to_all(packed, "rp", split_axis=0, concat_axis=0, tiled=True)

    vectors = rp_coords.shape[1]
    total = devices * per_device
    fourier = pl.pallas_call(
        fourier_kernel,
        out_shape=vmem((devices, 3, per_device, LANES), jnp.bfloat16),
        scratch_shapes=[
            pltpu.VMEM((total, 2 * vectors), jnp.bfloat16),
            pltpu.VMEM((2 * vectors, 3 * LANES), jnp.bfloat16),
        ],
        compiler_params=room(16),
        name="fourier",
    )(moved, turns_of)
    fourier, u_table, v_table, e_table = lax.optimization_barrier(
        (fourier, u_table, v_table, e_table)
    )
    owned = lax.all_to_all(fourier, AXES, split_axis=0, concat_axis=0, tiled=True)
    owned = owned.reshape(groups, columns, 3, per_device, LANES)

    return pl.pallas_call(
        rotate_kernel,
        out_shape=vmem((per_device, 2, BANDS, BANDS * BRANCHES), jnp.float32),
        scratch_shapes=[
            pltpu.VMEM((per_device, 2, BANDS, BANDS * BRANCHES), jnp.float32),
            pltpu.SemaphoreType.DMA((BANDS // 8,)),
        ],
        out_specs=pl.BlockSpec(memory_space=pl.ANY),
        compiler_params=room(16),
        name="rotate",
    )(owned, v_table, e_table, u_table)


def solution(mesh):
    return jax.shard_map(
        local,
        mesh=mesh,
        in_specs=(
            P(None, "rp", "pb", None),
            P(),
            P(None, AXES),
            P(),
            P(),
            P(AXES, None, None, None),
            P(AXES, None, None, None),
        ),
        out_specs=P(AXES, None, None, None),
        check_vma=False,
    )
```
